32 devices in a mesh: seq: 4 (over y, x), tp: 4 (over z), grp: 2 (over core).
Axes of the slice: x: 2, y: 2, z: 4, core: 2. Of those that a mesh axis runs over, the one named last changes fastest.
Arguments:
- query: bfloat16 [16, 64, 8192], P('grp', None, 'tp'), parts along dimension 0, may hold values from -15 to 15
- cache: bfloat16 [16, 4096, 8, 256], P('grp', 'tp', 'seq'), parts along dimension 0, may hold values from -6 to 6
- head_of_slot: int32 [16], P('grp'), parts along dimension 0, may hold values from 0 to 7, each once
- lengths: int32 [16], P('grp'), parts along dimension 0, may hold values from 2048 to 4096
- out_weight: bfloat16 [8192, 8192], P('tp', 'seq'), may hold values from -0.0625 to 0.0625
Outputs:
- projected: bfloat16 [16, 64, 8192], P(('grp', 'tp'), None, 'seq'), parts along dimension 0
The draws below stay inside these ranges and needn't reach their ends.
There are 2 independent parts, one for each index of `grp`. The reference program is written for one: setup_inputs(seed, part) draws one part's arguments, and reference() takes and returns one part's arrays. A program takes and returns all parts, laid end to end along the dimension named above; an argument that names none is the same for every part. Nothing has to cross between parts.
Inputs may be any that keep to these rules, and one draw needn't show every extreme that they name: head_of_slot names every KV head exactly once.
All inputs are finite; a program needn't handle non-finite values.
Results may differ from the reference program's by a relative error of at most 0.01.
Values may be sent and summed in bfloat16 or wider, within the bound.
A program may use at most 128 MiB of HBM per device.

```python
import math
import jax
import jax.numpy as jnp
from jax import lax

D = 8192
HQ = 64
KVH = 8
HD = 128
B = 8
QT = 64
L = 4096


def draw_query(key, part):
    own_key = jax.random.fold_in(key, 11)
    values = jnp.clip(3.0 * jax.random.normal(own_key, (B, QT, HQ * HD), jnp.float32), -15.0, 15.0)
    return values.astype(jnp.bfloat16)


def draw_cache(key, part):
    own_key = jax.random.fold_in(key, 23)
    values = jnp.clip(jax.random.normal(own_key, (B, L, KVH, 2 * HD), jnp.float32), -6.0, 6.0)
    return values.astype(jnp.bfloat16)


def with_ends(values, key, smallest, top_value):
    shape = values.shape
    spot = [jax.random.randint(jax.random.fold_in(key, axis), (), 0, shape[axis]) for axis in range(len(shape))]
    values = values.at[tuple(spot)].set(smallest)
    longest = shape.index(max(shape))
    spot[longest] = (spot[longest] + 1) % shape[longest]
    return values.at[tuple(spot)].set(top_value)


def shard_levels(stream_key, extent, shards, smallest, top_value):
    factor_of = 1.0
    for position, parts in shards:
        heights = jax.random.uniform(jax.random.fold_in(jax.random.fold_in(stream_key, 6), position), (parts,), jnp.float32, smallest / len(shards), top_value / len(shards))
        factor_of = factor_of * jnp.repeat(jnp.exp(heights), extent[position] // parts).reshape((-1,) + (1,) * (len(extent) - 1 - position))
    return factor_of


def noise(key, shape, spread, bound, cuts=(), kind=jnp.bfloat16):
    loudness = shard_levels(key, shape, cuts, -0.22, 0.18) if cuts else 1.0
    drawn = jax.random.normal(key, shape, jnp.float32) * spread * loudness
    return jnp.minimum(jnp.maximum(drawn, -bound), bound).astype(kind)


def setup_inputs(seed: int = 0, part: int = 0) -> dict:
    arg_keys = jax.random.split(jax.random.key(seed), 6)
    own_keys = jax.random.split(jax.random.fold_in(arg_keys[5], part), 6)
    query = draw_query(jax.random.fold_in(jax.random.fold_in(arg_keys[5], part), 71), part)
    cache = draw_cache(jax.random.fold_in(jax.random.fold_in(arg_keys[5], part), 71), part)
    head_of_slot = jax.random.permutation(own_keys[2], KVH).astype(jnp.int32)
    lengths = with_ends(jax.random.randint(own_keys[3], (B,), L // 2, L + 1), jax.random.fold_in(own_keys[3], 1), L // 2, L).astype(jnp.int32)
    out_weight = noise(arg_keys[4], (HQ * HD, D), (HQ * HD) ** -0.5, 0.0625, ((0, 4), (1, 4)))
    return dict(query=query, cache=cache, head_of_slot=head_of_slot, lengths=lengths, out_weight=out_weight)


MASKED_SCORE = -1e+30

def reference(query, cache, head_of_slot, lengths, out_weight):
    group_size = HQ // KVH
    scaling = 1.0 / math.sqrt(HD)
    slot_ids = jnp.arange(KVH, dtype=jnp.int32)
    slot_of_head = lax.optimization_barrier(jnp.sum(jnp.where(head_of_slot[None, :] == slot_ids[:, None], slot_ids[None, :], 0), axis=1)).astype(jnp.int32)
    positions = jnp.arange(L, dtype=jnp.int32)
    row_token = jnp.arange(QT * group_size, dtype=jnp.int32) // group_size

    def attend_pair(pair_index):
        seq_index = pair_index // KVH
        kv_head = pair_index % KVH
        entries = lax.dynamic_index_in_dim(cache, seq_index, 0, False)
        entries = lax.dynamic_index_in_dim(entries, slot_of_head[kv_head], 1, False)
        queries = lax.dynamic_index_in_dim(query, seq_index, 0, False)
        queries = lax.dynamic_slice_in_dim(queries, kv_head * group_size * HD, group_size * HD, 1)
        queries = queries.reshape(QT * group_size, HD)
        scores = jnp.dot(queries, entries[:, :HD].T, preferred_element_type=jnp.float32) * scaling
        limits = lengths[seq_index] - QT + row_token
        visible = positions[None, :] <= limits[:, None]
        scores = jnp.where(visible, scores, MASKED_SCORE)
        maxima = lax.optimization_barrier(jnp.max(scores, axis=1))
        weights = jnp.where(visible, jnp.exp(scores - maxima[:, None]), 0.0)
        totals = lax.optimization_barrier(jnp.sum(weights, axis=1))
        blended = jnp.dot(weights.astype(jnp.bfloat16), entries[:, HD:], preferred_element_type=jnp.float32)
        return (blended / totals[:, None]).astype(jnp.bfloat16).reshape(QT, group_size * HD)
    attended = lax.map(attend_pair, jnp.arange(B * KVH, dtype=jnp.int32))
    attended = attended.reshape(B, KVH, QT, group_size * HD).transpose(0, 2, 1, 3).reshape(B * QT, HQ * HD)
    projected = jnp.dot(attended, out_weight, preferred_element_type=jnp.float32)
    return projected.astype(jnp.bfloat16).reshape(B, QT, D)
```

```python
import functools
import math

import jax
import jax.numpy as jnp
from jax import lax
from jax.experimental import pallas as pl
from jax.experimental.pallas import tpu as pltpu
from jax.sharding import PartitionSpec as P

HQ = 64
KVH = 8
CHUNKS = 2
TOKEN_CUTS = 2
PERIOD = 2.0
AFTER = (0.0, 0.4, 0.8, 2.4, 3.9, 5.2, 6.2, 7.3, 8.7, 9.5)
SPLIT_AT = (-0.1, 0.05, 0.3, 0.5, 1.6, 1.7, 3.3, 3.4)
MASKED_SCORE = -1e30
FLOOR = -1e29
MESH = pl.DeviceIdType.MESH


def slot_table(head_of_slot):
    slot_total = head_of_slot.shape[0]
    slot_ids = jnp.arange(slot_total, dtype=jnp.int32)
    return jnp.sum(
        jnp.where(head_of_slot[None, :] == slot_ids[:, None], slot_ids[None, :], 0), axis=1
    )


def greet(axes):
    barrier = pltpu.get_barrier_semaphore()
    total = 0
    for axis in axes:
        n = lax.axis_size(axis)
        me = lax.axis_index(axis)
        for k in range(1, n):
            pl.semaphore_signal(
                barrier, inc=1, device_id={axis: lax.rem(me + k, n)}, device_id_type=MESH
            )
            total += 1
    pl.semaphore_wait(barrier, total)


def remote(src, dst, send_sem, recv_sem, axis, k):
    n = lax.axis_size(axis)
    target = lax.rem(lax.axis_index(axis) + k, n)
    return pltpu.make_async_remote_copy(
        src_ref=src,
        dst_ref=dst,
        send_sem=send_sem,
        recv_sem=recv_sem,
        device_id={axis: target},
        device_id_type=MESH,
    )


def back(axis, index):
    n = lax.axis_size(axis)
    return lax.rem(lax.axis_index(axis) + n - index, n)


def gather_attend_kernel(
    dims, hos, lens, q_ref, kv_hbm, att_ref,
    raw, kv_ref, kv_sem, zq, xs, xr, osend, orecv, lsend, lrecv, scores,
    zq_s, zq_r, xq_s, xq_r, o_s, o_r, l_s, l_r, own_sem,
):
    nc, bq, nsq, hl, ns, per_tp, Lb, hd, G, T = dims
    n_tp, n_seq = lax.axis_size("tp"), lax.axis_size("seq")
    me_t, me_s = lax.axis_index("tp"), lax.axis_index("seq")
    rows = G * T
    block = math.gcd(Lb, 256)
    scale = math.log2(math.e) / math.sqrt(hd)
    fetch = pltpu.make_async_copy(kv_hbm, raw, kv_sem)
    fetch.start()
    greet(("tp", "seq"))

    zsends = [
        [remote(q_ref.at[c], zq[c].at[k], zq_s.at[c, k], zq_r.at[c, k], "tp", k) for k in range(1, n_tp)]
        for c in range(nc)
    ]
    owns = [pltpu.make_async_copy(q_ref.at[c], zq[c].at[0], own_sem.at[c]) for c in range(nc)]
    for c in range(nc):
        for copy in zsends[c]:
            copy.start()
        owns[c].start()

    xsends = [
        [remote(xs.at[c, k], xr.at[c, k], xq_s.at[c, k], xq_r.at[c, k], "seq", k) for k in range(1, n_seq)]
        for c in range(nc)
    ]

    def spread(c):
        owns[c].wait()
        for copy in zsends[c]:
            copy.wait_recv()
        for k in list(range(1, n_seq)) + [0]:
            target = xr if k == 0 else xs
            column = lax.rem(me_s + k, n_seq)
            for j in range(ns):
                head = hos[column * ns + j]
                target[c, k, j] = zq[c][back("tp", head // hl), head % hl]
            if k:
                xsends[c][k - 1].start()

    osends = [
        [remote(osend.at[c, k], orecv.at[c, k], o_s.at[c, k], o_r.at[c, k], "tp", k) for k in range(1, n_tp)]
        for c in range(nc)
    ]
    lsends = [
        [remote(lsend.at[c, k], lrecv.at[c, k], l_s.at[c, k], l_r.at[c, k], "tp", k) for k in range(1, n_tp)]
        for c in range(nc)
    ]

    def attend_pair(c, k, pair):
        x, slot = pair // ns, pair % ns
        plane = lax.rem(me_t + k, n_tp)
        local_seq = plane * bq + x
        whole_seq = plane * per_tp + c * bq + x
        source = back("seq", local_seq // nsq)
        queries = xr[c, source, slot, local_seq % nsq].reshape(rows, hd)
        visible_end = lens[whole_seq] - me_t * Lb
        limits = visible_end - T + lax.broadcasted_iota(jnp.int32, (1, rows), 1) % T
        top = jnp.full((1, rows), FLOOR, jnp.float32)
        for i in range(Lb // block):
            s = lax.dot_general(
                kv_ref[slot, whole_seq, i * block : (i + 1) * block, :hd],
                queries,
                (((1,), (1,)), ((), ())),
                preferred_element_type=jnp.float32,
            )
            pos = i * block + lax.broadcasted_iota(jnp.int32, (block, 1), 0)
            s = jnp.where(pos <= limits, s * scale, MASKED_SCORE)
            scores[i * block : (i + 1) * block, :] = s
            top = jnp.maximum(top, jnp.max(s, axis=0, keepdims=True))
        total = jnp.zeros((1, rows), jnp.float32)
        out = jnp.zeros((hd, rows), jnp.float32)
        for i in range(Lb // block):
            w = jnp.exp2(scores[i * block : (i + 1) * block, :] - top)
            total = total + jnp.sum(w, axis=0, keepdims=True)
            out = out + lax.dot_general(
                kv_ref[slot, whole_seq, i * block : (i + 1) * block, hd:],
                w.astype(jnp.bfloat16),
                (((0,), (0,)), ((), ())),
                preferred_element_type=jnp.float32,
            )
        total = jnp.maximum(total, 1e-30)
        o_to, l_to = (orecv, lrecv) if k == 0 else (osend, lsend)
        o_to[c, k, x, slot] = (out / total).astype(jnp.bfloat16)
        l_to[c, k, x, slot] = top + jnp.log2(total)

    def attend(c):
        for copy in xsends[c]:
            copy.wait_recv()
        order = sorted(range(1, n_tp), key=lambda k: abs(k - n_tp / 2)) + [0]
        for k in order:
            lax.fori_loop(0, bq * ns, lambda pair, _: (attend_pair(c, k, pair), 0)[1], 0)
            if k:
                osends[c][k - 1].start()
                lsends[c][k - 1].start()

    def merge(c):
        for k in range(n_tp - 1):
            osends[c][k].wait_recv()
            lsends[c][k].wait_recv()

        def one(pair, _):
            x, slot = pair // ns, pair % ns
            ls = [lrecv[c, k, x, slot] for k in range(n_tp)]
            top = functools.reduce(jnp.maximum, ls)
            ws = [jnp.exp2(l - top) for l in ls]
            inverse = 1.0 / sum(ws)
            out = jnp.zeros((hd, rows), jnp.float32)
            for k in range(n_tp):
                out = out + (ws[k] * inverse) * orecv[c, k, x, slot].astype(jnp.float32)
            att_ref[c, x, slot] = out.astype(jnp.bfloat16)
            return 0

        lax.fori_loop(0, bq * ns, one, 0)

    fetch.wait()
    step = math.gcd(Lb, 128)
    turns = Lb // step

    def split(turn, _):
        at = pl.ds(pl.multiple_of(turn % turns * step, step), step)
        for slot in range(ns):
            kv_ref[slot, turn // turns, at, :] = raw[turn // turns, at, slot, :]
        return 0

    lax.fori_loop(0, raw.shape[0] * turns, split, 0)
    for c in range(nc):
        spread(c)
        if c:
            attend(c - 1)
    attend(nc - 1)
    for c in range(nc):
        merge(c)
    for c in range(nc):
        for copy in zsends[c] + xsends[c] + osends[c] + lsends[c]:
            copy.wait_send()


def gather_attend(qm, kv, head_of_slot, lengths, dims):
    nc, bq, nsq, hl, ns, per_tp, Lb, hd, G, T = dims
    n_tp, n_seq = lax.axis_size("tp"), lax.axis_size("seq")
    rows = G * T
    bf, f32 = jnp.bfloat16, jnp.float32
    dma = pltpu.SemaphoreType.DMA
    vmem = pl.BlockSpec(memory_space=pltpu.VMEM)
    smem = pl.BlockSpec(memory_space=pltpu.SMEM)
    return pl.pallas_call(
        functools.partial(gather_attend_kernel, dims),
        out_shape=jax.ShapeDtypeStruct((nc, bq, ns, hd, rows), bf),
        in_specs=[smem, smem, vmem, pl.BlockSpec(memory_space=pl.ANY)],
        out_specs=vmem,
        scratch_shapes=[
            pltpu.VMEM(kv.shape, bf),
            pltpu.VMEM((ns, kv.shape[0], Lb, 2 * hd), bf),
            dma(()),
            [pltpu.VMEM((n_tp, hl, nsq, G, T, hd), bf)] * nc,
            pltpu.VMEM((nc, n_seq, ns, nsq, G, T, hd), bf),
            pltpu.VMEM((nc, n_seq, ns, nsq, G, T, hd), bf),
            pltpu.VMEM((nc, n_tp, bq, ns, hd, rows), bf),
            pltpu.VMEM((nc, n_tp, bq, ns, hd, rows), bf),
            pltpu.VMEM((nc, n_tp, bq, ns, 1, rows), f32),
            pltpu.VMEM((nc, n_tp, bq, ns, 1, rows), f32),
            pltpu.VMEM((Lb, rows), f32),
            dma((nc, n_tp)), dma((nc, n_tp)), dma((nc, n_seq)), dma((nc, n_seq)),
            dma((nc, n_tp)), dma((nc, n_tp)), dma((nc, n_tp)), dma((nc, n_tp)), dma((nc,)),
        ],
        compiler_params=pltpu.CompilerParams(
            collective_id=0, has_side_effects=True, vmem_limit_bytes=56 * 2**20
        ),
    )(head_of_slot, lengths, qm, kv)


def project_kernel(
    dims, soh, att_ref, w_hbm, out_ref,
    w_ref, xr, zs, zr, ag, own, ps, pr,
    x_s, x_r, z_s, z_r, a_s, a_r, p_s, p_r, w_sem, own_sem,
):
    nc, bq, hl, ns, sub, part, T = dims
    n_tp, n_seq = lax.axis_size("tp"), lax.axis_size("seq")
    me_t, me_s = lax.axis_index("tp"), lax.axis_index("seq")
    width, columns = w_ref.shape
    few = bq * sub
    load = pltpu.make_async_copy(w_hbm, w_ref, w_sem)
    greet(("tp", "seq"))
    xsends = [
        [
            remote(att_ref.at[c, lax.rem(me_s + k, n_seq)], xr[c].at[k], x_s.at[c, k], x_r.at[c, k], "seq", k)
            for k in range(1, n_seq)
        ]
        for c in range(nc)
    ]
    owns = [pltpu.make_async_copy(att_ref.at[c, me_s], xr[c].at[0], own_sem.at[c]) for c in range(nc)]
    for c in range(nc):
        for copy in xsends[c]:
            copy.start()
        owns[c].start()
    load.start()
    zsends = [
        [remote(zs.at[c, k], zr.at[c, k], z_s.at[c, k], z_r.at[c, k], "tp", k) for k in range(1, n_tp)]
        for c in range(nc)
    ]
    asends = [
        [remote(zr.at[c], ag.at[c, k], a_s.at[c, k], a_r.at[c, k], "seq", k) for k in range(1, n_seq)]
        for c in range(nc)
    ]
    psends = [
        [remote(ps.at[c, k], pr.at[c, k], p_s.at[c, k], p_r.at[c, k], "tp", k) for k in range(1, n_tp)]
        for c in range(nc)
    ]
    for c in range(nc):
        owns[c].wait()
        for copy in xsends[c]:
            copy.wait_recv()
        for k in list(range(1, n_tp)) + [0]:
            target = zr if k == 0 else zs
            plane = lax.rem(me_t + k, n_tp)
            for j in range(hl):
                slot = soh[plane * hl + j]
                picked = xr[c][back("seq", slot // ns), slot % ns]
                target[c, k, :, j * part : (j + 1) * part] = picked
            if k:
                zsends[c][k - 1].start()
    for c in range(nc):
        for copy in zsends[c]:
            copy.wait_recv()
        for copy in asends[c]:
            copy.start()
    load.wait()
    tile = math.gcd(columns, 512)
    for c in range(nc):
        for copy in asends[c]:
            copy.wait_recv()
        pieces = []
        for k in range(n_tp):
            j = (n_tp - k) % n_tp
            for p in range(n_seq):
                pieces.append(zr[c, j] if p == 0 else ag[c, p, j])
        rows = jnp.concatenate(pieces, axis=0)

        def column_tile(i, _):
            at = pl.ds(pl.multiple_of(i * tile, tile), tile)
            product = jnp.dot(rows, w_ref[:, at], preferred_element_type=jnp.float32)
            span = n_seq * few
            own[c, :, at] = product[:span]
            for k in range(1, n_tp):
                ps[c, k, :, at] = product[k * span : (k + 1) * span].astype(jnp.bfloat16)
            return 0

        lax.fori_loop(0, columns // tile, column_tile, 0)
        for copy in psends[c]:
            copy.start()
    for c in range(nc):
        for copy in psends[c]:
            copy.wait_recv()
        for p in range(n_seq):
            column = lax.rem(me_s + n_seq - p, n_seq)
            for x in range(bq):
                at = p * few + x * sub
                total = own[c, at : at + sub]
                for k in range(1, n_tp):
                    total = total + pr[c, k, at : at + sub].astype(jnp.float32)
                out_ref[c * bq + x, pl.ds(pl.multiple_of(column * sub, sub), sub)] = total.astype(jnp.bfloat16)
    for c in range(nc):
        for copy in xsends[c] + zsends[c] + asends[c] + psends[c]:
            copy.wait_send()


def project(att, weight, slot_of_head, dims):
    nc, bq, hl, ns, sub, part, T = dims
    n_tp, n_seq = lax.axis_size("tp"), lax.axis_size("seq")
    width, columns = weight.shape
    few = bq * sub
    bf, f32 = jnp.bfloat16, jnp.float32
    dma = pltpu.SemaphoreType.DMA
    vmem = pl.BlockSpec(memory_space=pltpu.VMEM)
    return pl.pallas_call(
        functools.partial(project_kernel, dims),
        out_shape=jax.ShapeDtypeStruct((nc * bq, T, columns), bf),
        in_specs=[
            pl.BlockSpec(memory_space=pltpu.SMEM), vmem, pl.BlockSpec(memory_space=pl.ANY)
        ],
        out_specs=vmem,
        scratch_shapes=[
            pltpu.VMEM((width, columns), bf),
            [pltpu.VMEM((n_seq, ns, few, part), bf)] * nc,
            pltpu.VMEM((nc, n_tp, few, width), bf),
            pltpu.VMEM((nc, n_tp, few, width), bf),
            pltpu.VMEM((nc, n_seq, n_tp, few, width), bf),
            pltpu.VMEM((nc, n_seq * few, columns), f32),
            pltpu.VMEM((nc, n_tp, n_seq * few, columns), bf),
            pltpu.VMEM((nc, n_tp, n_seq * few, columns), bf),
            dma((nc, n_seq)), dma((nc, n_seq)), dma((nc, n_tp)), dma((nc, n_tp)),
            dma((nc, n_seq)), dma((nc, n_seq)), dma((nc, n_tp)), dma((nc, n_tp)),
            dma(()), dma((nc,)),
        ],
        compiler_params=pltpu.CompilerParams(
            collective_id=1, has_side_effects=True, vmem_limit_bytes=48 * 2**20
        ),
    )(slot_of_head, att, weight)


def line_kernel(
    dims, hos, lens, q_hbm, kv_hbm, w_hbm, out_ref,
    raw, kv_ref, w_ref, az, xs, xr, osend, orecv, lsend, lrecv, scores,
    bs, bls, bm, blm, br, blr, xg, own, ds, dm, dr,
    kv_sem, w_sem, q_sem,
    a_s, a_r, xq_s, xq_r, o_s, o_r, l_s, l_r,
    b_s, b_r, bl_s, bl_r, g_s, g_r, d_s, d_r,
):
    nth, tt, hl, ns, Lb, hd, G = dims
    n_tp, n_seq = lax.axis_size("tp"), lax.axis_size("seq")
    me_t, me_s = lax.axis_index("tp"), lax.axis_index("seq")
    per_tp = out_ref.shape[0]
    nc = per_tp * nth
    T = nth * tt
    rows = G * tt
    columns = w_ref.shape[1]
    half = me_t // 2
    partner = me_t + 1 - 2 * (me_t % 2)
    far_inner = 2 - half
    far_outer = 3 - 3 * half
    inner = me_t == 1 + half
    outer = me_t == 3 * half
    block = math.gcd(Lb, 256)
    scale = math.log2(math.e) / math.sqrt(hd)
    bf, f32 = jnp.bfloat16, jnp.float32

    def part(c):
        return c // nth, c % nth

    def to(axis, target, src, dst, send, recv):
        return pltpu.make_async_remote_copy(
            src_ref=src, dst_ref=dst, send_sem=send, recv_sem=recv,
            device_id={axis: target}, device_id_type=MESH,
        )

    def ring(target_of):
        return [[target_of(c, k) for k in range(1, n_seq)] for c in range(nc)]

    def block_to(c, i, plane, target):
        return to("tp", target, az[c].at[plane], az[c].at[plane], a_s.at[c, i], a_r.at[c, i])

    own_p = [block_to(c, 0, me_t, partner) for c in range(nc)]
    own_f = [block_to(c, 1, me_t, far_inner) for c in range(nc)]
    via_f = [block_to(c, 2, partner, far_inner) for c in range(nc)]
    via_a = [block_to(c, 3, far_inner, partner) for c in range(nc)]
    via_b = [block_to(c, 4, far_outer, partner) for c in range(nc)]
    column = lambda k: lax.rem(me_s + k, n_seq)
    xsends = ring(lambda c, k: to("seq", column(k), xs.at[c, k], xr.at[c, k], xq_s.at[c, k], xq_r.at[c, k]))
    osends = ring(lambda c, k: to("seq", column(k), osend.at[c, k], orecv[c].at[k], o_s.at[c, k], o_r.at[c, k]))
    lsends = ring(lambda c, k: to("seq", column(k), lsend.at[c, k], lrecv[c].at[k], l_s.at[c, k], l_r.at[c, k]))
    gsends = ring(lambda c, k: to("seq", column(k), xg.at[c, 0], xg.at[c, k], g_s.at[c, k], g_r.at[c, k]))

    def swap(c, send, mid, out, s, r):
        return dict(
            pair=to("tp", partner, send.at[c, 0], out.at[c, 0], s.at[c, 0], r.at[c, 0]),
            lift=[to("tp", partner, send.at[c, i], mid.at[c, i - 1], s.at[c, i], r.at[c, i]) for i in (1, 2)],
            cross=[
                to("tp", target, send.at[c, i], out.at[c, 1], s.at[c, 2 + i], r.at[c, 3])
                for i, target in ((1, far_inner), (2, far_outer))
            ],
        )

    bz = [(swap(c, bs, bm, br, b_s, b_r), swap(c, bls, blm, blr, bl_s, bl_r)) for c in range(nc)]
    dz = [(swap(c, ds, dm, dr, d_s, d_r),) for c in range(nc)]

    def own_blocks(c):
        x, th = part(c)
        for j in range(hl):
            for g in range(G):
                yield pltpu.make_async_copy(
                    q_hbm.at[me_s * per_tp + x, pl.ds(th * tt, tt), pl.ds((j * G + g) * hd, hd)],
                    az[c].at[me_t, j, g],
                    q_sem.at[c],
                )

    def ask_own(c):
        pltpu.make_async_copy(az[c].at[me_t], az[c].at[me_t], q_sem.at[c]).wait()
        own_p[c].start()

        @pl.when(inner)
        def _():
            own_f[c].start()

    def relay_a(c):
        @pl.when(inner)
        def _():
            own_p[c].wait_recv()
            via_f[c].start()
            own_f[c].wait_recv()
            via_a[c].start()

    def relay_b(c):
        @pl.when(inner)
        def _():
            via_f[c].wait_recv()
            via_b[c].start()

    def spread(c):
        @pl.when(outer)
        def _():
            own_p[c].wait_recv()
            via_a[c].wait_recv()
            via_b[c].wait_recv()

        for k in list(range(1, n_seq)) + [0]:
            target = xr if k == 0 else xs
            for j in range(ns):
                head = hos[column(k) * ns + j]
                target[c, k, j] = az[c][head // hl, head % hl]
            if k:
                xsends[c][k - 1].start()

    def attend_pair(c, k, slot):
        x, th = part(c)
        seq = column(k) * per_tp + x
        queries = xr[c, (n_seq - k) % n_seq, slot].reshape(rows, hd)
        visible_end = lens[seq] - me_t * Lb
        limits = visible_end - T + th * tt + lax.broadcasted_iota(jnp.int32, (1, rows), 1) % tt
        top = jnp.full((1, rows), FLOOR, f32)
        for i in range(Lb // block):
            s = lax.dot_general(
                kv_ref[slot, seq, i * block : (i + 1) * block, :hd],
                queries,
                (((1,), (1,)), ((), ())),
                preferred_element_type=f32,
            )
            pos = i * block + lax.broadcasted_iota(jnp.int32, (block, 1), 0)
            s = jnp.where(pos <= limits, s * scale, MASKED_SCORE)
            scores[i * block : (i + 1) * block, :] = s
            top = jnp.maximum(top, jnp.max(s, axis=0, keepdims=True))
        total = jnp.zeros((1, rows), f32)
        out = jnp.zeros((hd, rows), f32)
        for i in range(Lb // block):
            w = jnp.exp2(scores[i * block : (i + 1) * block, :] - top)
            total = total + jnp.sum(w, axis=0, keepdims=True)
            out = out + lax.dot_general(
                kv_ref[slot, seq, i * block : (i + 1) * block, hd:],
                w.astype(bf),
                (((0,), (0,)), ((), ())),
                preferred_element_type=f32,
            )
        total = jnp.maximum(total, 1e-30)
        o_to = orecv[c].at[0] if k == 0 else osend.at[c, k]
        l_to = lrecv[c].at[0] if k == 0 else lsend.at[c, k]
        o_to[slot] = (out / total).astype(bf)
        l_to[slot] = top + jnp.log2(total)

    def attend(c):
        for copy in xsends[c]:
            copy.wait_recv()
        for k in list(range(1, n_seq)) + [0]:
            lax.fori_loop(0, ns, lambda slot, _: (attend_pair(c, k, slot), 0)[1], 0)
            if k:
                osends[c][k - 1].start()
                lsends[c][k - 1].start()

    def picked(c, plane, j):
        head = plane * hl + j
        slot = jnp.int32(0)
        for s in range(n_seq * ns):
            slot = jnp.maximum(slot, jnp.where(hos[s] == head, s, 0))
        k = lax.rem(me_s + n_seq - slot // ns, n_seq)
        return orecv[c][k, slot % ns], lrecv[c][k, slot % ns]

    def merged(parts):
        top = functools.reduce(jnp.maximum, [l for _, l in parts])
        ws = [jnp.exp2(l - top) for _, l in parts]
        total = functools.reduce(jnp.add, ws)
        inverse = 1.0 / total
        out = functools.reduce(
            jnp.add, [(w * inverse) * o.astype(f32) for w, (o, _) in zip(ws, parts)]
        )
        return out, top + jnp.log2(total)

    def put(c, i, plane):
        for j in range(hl):
            o, l = picked(c, plane, j)
            bs[c, i, j] = o
            bls[c, i, j] = l

    def part_send(c):
        for copy in osends[c] + lsends[c]:
            copy.wait_recv()

        @pl.when(outer)
        def _():
            for i, plane in ((1, far_inner), (2, far_outer)):
                put(c, i, plane)
                for z in bz[c]:
                    z["lift"][i - 1].start()

        put(c, 0, partner)
        for z in bz[c]:
            z["pair"].start()

    def part_join(c):
        @pl.when(inner)
        def _():
            for i, plane in ((2, far_outer), (1, far_inner)):
                for z in bz[c]:
                    z["lift"][i - 1].wait_recv()
                for j in range(hl):
                    o, l = merged([picked(c, plane, j), (bm[c, i - 1, j], blm[c, i - 1, j])])
                    bs[c, i, j] = o.astype(bf)
                    bls[c, i, j] = l
                for z in bz[c]:
                    z["cross"][i - 1].start()

    def part_end(c):
        for z in bz[c]:
            z["pair"].wait_recv()
            z["cross"][0].wait_recv()
        for j in range(hl):
            o, _ = merged([picked(c, me_t, j)] + [(br[c, i, j], blr[c, i, j]) for i in range(2)])
            turned = o.T.astype(bf)
            for g in range(G):
                at = (j * G + g) * hd
                xg[c, 0, :, at : at + hd] = turned[g * tt : (g + 1) * tt]
        for copy in gsends[c]:
            copy.start()

    tile = math.gcd(columns, 512)

    def project(c):
        for copy in gsends[c]:
            copy.wait_recv()
        planes = [me_t, partner, far_inner, far_outer]
        lhs = jnp.concatenate(
            [xg[c, lax.rem(me_s + n_seq - p, n_seq)] for p in planes], axis=0
        )

        def column_tile(i, _):
            at = pl.ds(pl.multiple_of(i * tile, tile), tile)
            product = jnp.dot(lhs, w_ref[:, at], preferred_element_type=f32)
            own[c, :, at] = product[:tt]
            for i in range(3):
                ds[c, i, :, at] = product[(i + 1) * tt : (i + 2) * tt].astype(bf)
            return 0

        lax.fori_loop(0, columns // tile, column_tile, 0)

        @pl.when(outer)
        def _():
            for copy in dz[c][0]["lift"]:
                copy.start()

        dz[c][0]["pair"].start()

    def sum_join(c):
        z = dz[c][0]

        @pl.when(inner)
        def _():
            for i in (2, 1):
                z["lift"][i - 1].wait_recv()
                ds[c, i] = (ds[c, i].astype(f32) + dm[c, i - 1].astype(f32)).astype(bf)
                z["cross"][i - 1].start()

    def sum_end(c):
        x, th = part(c)
        z = dz[c][0]
        z["pair"].wait_recv()
        z["cross"][0].wait_recv()
        total = own[c] + dr[c, 0].astype(f32) + dr[c, 1].astype(f32)
        out_ref[x, th * tt : (th + 1) * tt] = total.astype(bf)

    step = math.gcd(Lb, 128)
    turns = Lb // step
    n_b = raw.shape[0]
    seq_order = [p * per_tp + x for x in range(per_tp) for p in range(n_tp)]
    fetches = [pltpu.make_async_copy(kv_hbm.at[b], raw.at[b], kv_sem.at[b]) for b in range(n_b)]

    def split(index):
        b = seq_order[index]
        fetches[b].wait()

        def turn(i, _):
            at = pl.ds(pl.multiple_of(i * step, step), step)
            for slot in range(ns):
                kv_ref[slot, b, at, :] = raw[b, at, slot, :]
            return 0

        lax.fori_loop(0, turns, turn, 0)

    load = pltpu.make_async_copy(w_hbm, w_ref, w_sem)

    for c in range(nc):
        for copy in own_blocks(c):
            copy.start()
    for b in seq_order:
        fetches[b].start()
    load.start()
    greet(("tp", "seq"))

    run = dict(
        q=ask_own, ra=relay_a, rb=relay_b, sp=spread, at=attend, bs=part_send, bj=part_join,
        be=part_end, pr=project, dj=sum_join, de=sum_end, kv=split, w=lambda _: load.wait(),
    )
    for name, c in order_of(nc, n_b):
        run[name](c)

    for c in range(nc):
        own_p[c].wait_send()
        for copy in xsends[c] + osends[c] + lsends[c] + gsends[c]:
            copy.wait_send()
        for z in bz[c] + dz[c]:
            z["pair"].wait_send()

        @pl.when(outer)
        def _():
            for z in bz[c] + dz[c]:
                for copy in z["lift"]:
                    copy.wait_send()

        @pl.when(inner)
        def _():
            for copy in (own_f[c], via_f[c], via_a[c], via_b[c]):
                copy.wait_send()
            for z in bz[c] + dz[c]:
                for copy in z["cross"]:
                    copy.wait_send()


def order_of(nc, n_b):
    steps = ["ra", "rb", "sp", "at", "bs", "bj", "be", "pr", "dj", "de"]
    after = dict(zip(steps, AFTER))
    plan = []
    for c in range(nc):
        for place, name in enumerate(steps):
            plan.append((c * PERIOD + after[name], place, name, c))
        if c:
            plan.append(((c - 1) * PERIOD + after["ra"] + 0.1, 0, "q", c))
    for i in range(n_b):
        plan.append((SPLIT_AT[i * len(SPLIT_AT) // n_b], 0, "kv", i))
    plan.append((after["pr"] - 0.01, 0, "w", 0))
    return [("q", 0)] + [(name, c) for _, _, name, c in sorted(plan, key=lambda e: (e[0], -e[1]))]


def line_call(query, cache, head_of_slot, lengths, out_weight, nth):
    n_seq, n_tp = lax.axis_size("seq"), lax.axis_size("tp")
    G = HQ // KVH
    B, T, _ = query.shape
    Lb, ns, hd2 = cache.shape[1:]
    hd = hd2 // 2
    hl = KVH // n_tp
    per_tp = B // n_tp
    tt = T // nth
    nc = per_tp * nth
    rows = G * tt
    columns = out_weight.shape[1]
    bf, f32 = jnp.bfloat16, jnp.float32
    dma = pltpu.SemaphoreType.DMA
    v = pltpu.VMEM
    anywhere = pl.BlockSpec(memory_space=pl.ANY)
    smem = pl.BlockSpec(memory_space=pltpu.SMEM)
    return pl.pallas_call(
        functools.partial(line_kernel, (nth, tt, hl, ns, Lb, hd, G)),
        out_shape=jax.ShapeDtypeStruct((per_tp, T, columns), bf),
        in_specs=[smem, smem, anywhere, anywhere, anywhere],
        out_specs=pl.BlockSpec(memory_space=pltpu.VMEM),
        scratch_shapes=[
            v(cache.shape, bf),
            v((ns, B, Lb, 2 * hd), bf),
            v(out_weight.shape, bf),
            [v((n_tp, hl, G, tt, hd), bf)] * nc,
            v((nc, n_seq, ns, G, tt, hd), bf),
            v((nc, n_seq, ns, G, tt, hd), bf),
            v((nc, n_seq, ns, hd, rows), bf),
            [v((n_seq, ns, hd, rows), bf)] * nc,
            v((nc, n_seq, ns, 1, rows), f32),
            [v((n_seq, ns, 1, rows), f32)] * nc,
            v((Lb, rows), f32),
            v((nc, 3, hl, hd, rows), bf), v((nc, 3, hl, 1, rows), f32),
            v((nc, 2, hl, hd, rows), bf), v((nc, 2, hl, 1, rows), f32),
            v((nc, 2, hl, hd, rows), bf), v((nc, 2, hl, 1, rows), f32),
            v((nc, n_seq, tt, hl * G * hd), bf),
            v((nc, tt, columns), f32),
            v((nc, 3, tt, columns), bf), v((nc, 2, tt, columns), bf), v((nc, 2, tt, columns), bf),
            dma((B,)), dma(()), dma((nc,)),
            dma((nc, 5)), dma((nc, 5)),
            dma((nc, n_seq)), dma((nc, n_seq)),
            dma((nc, n_seq)), dma((nc, n_seq)), dma((nc, n_seq)), dma((nc, n_seq)),
            dma((nc, 5)), dma((nc, 4)), dma((nc, 5)), dma((nc, 4)),
            dma((nc, n_seq)), dma((nc, n_seq)),
            dma((nc, 5)), dma((nc, 4)),
        ],
        compiler_params=pltpu.CompilerParams(
            collective_id=2, has_side_effects=True, vmem_limit_bytes=60 * 2**20
        ),
    )(head_of_slot, lengths, query, cache, out_weight)


def local(query, cache, head_of_slot, lengths, out_weight):
    G = HQ // KVH
    n_seq, n_tp = lax.axis_size("seq"), lax.axis_size("tp")
    me_s = lax.axis_index("seq")
    slot_of_head = slot_table(head_of_slot)
    B, T, width = query.shape
    Lb, ns, hd2 = cache.shape[1:]
    hd = hd2 // 2
    hl = KVH // n_tp
    per_tp = B // n_tp
    nth = math.gcd(TOKEN_CUTS, T)
    if n_tp == n_seq == 4 and HQ * hd == n_tp * width and T // nth % 16 == 0:
        return line_call(query, cache, head_of_slot, lengths, out_weight, nth)
    nc = math.gcd(CHUNKS, per_tp)
    bq = per_tp // nc
    nsq = n_tp * bq // n_seq
    sub = T // n_seq

    chunked = query.reshape(n_tp, nc, bq, T, width).transpose(1, 0, 2, 3, 4)
    chunked = chunked.reshape(nc, n_seq, nsq, T, width)
    mine = lax.dynamic_index_in_dim(chunked, me_s, 1, False)
    qm = mine.reshape(nc, nsq, T, hl, G, hd).transpose(0, 3, 1, 4, 2, 5)
    kv = cache
    att = gather_attend(
        qm, kv, head_of_slot, lengths, (nc, bq, nsq, hl, ns, per_tp, Lb, hd, G, T)
    )
    att = att.reshape(nc, bq, ns, hd, G, n_seq, sub).transpose(0, 5, 2, 1, 6, 4, 3)
    att = att.reshape(nc, n_seq, ns, bq * sub, G * hd)
    return project(att, out_weight, slot_of_head, (nc, bq, hl, ns, sub, G * hd, T))


def solution(mesh):
    in_specs = (
        P("grp", None, "tp"),
        P("grp", "tp", "seq", None),
        P("grp"),
        P("grp"),
        P("tp", "seq"),
    )
    out_specs = P(("grp", "tp"), None, "seq")
    return jax.shard_map(local, mesh=mesh, in_specs=in_specs, out_specs=out_specs, check_vma=False)
```

```python
import functools
import math

import jax
import jax.numpy as jnp
from jax import lax
from jax.experimental import pallas as pl
from jax.experimental.pallas import tpu as pltpu
from jax.sharding import PartitionSpec as P

HQ = 64
KVH = 8
CHUNKS = 2
CUTS = ((16, 32, 16), (16, 32, 16))
ORDER = (
    "q.0", "q.1", "kv.0", "ra.0", "kv.1", "ra.1", "kv.2", "rb.0", "kv.3", "rb.1", "q.5", "q.2",
    "kv.4", "sp.0", "q.4", "a0.0", "sp.1", "a0.1", "ra.2", "a1.0", "a2.0", "ra.4", "kv.5", "a1.1",
    "rb.2", "a3.0", "a2.1", "q.3", "rb.4", "ra.5", "sp.2", "a3.1", "bs.0", "kv.6", "sp.4", "bj.0",
    "a0.2", "ra.3", "kv.7", "rb.5", "bs.1", "a0.4", "a1.2", "a2.2", "a3.2", "be.0", "bj.1",
    "a1.4", "rb.3", "a2.4", "bs.2", "a3.4", "pr.0", "be.1", "sp.5", "bj.2", "sp.3", "a0.3",
    "bs.4", "dj.0", "pr.1", "a0.5", "a1.5", "a2.5", "bj.4", "a1.3", "a2.3", "a3.5", "a3.3",
    "dj.1", "bs.5", "be.2", "bs.3", "be.4", "pr.2", "bj.3", "bj.5", "pr.4", "dj.2", "be.3",
    "be.5", "dj.4", "de.1", "pr.3", "de.0", "pr.5", "dj.3", "de.4", "de.2", "dj.5", "de.3",
    "de.5",
)
FIRST_PROJECT = next(e for e in ORDER if e[:2] == "pr")
MASKED_SCORE = -1e30
FLOOR = -1e29
MESH = pl.DeviceIdType.MESH


def slot_table(head_of_slot):
    slot_total = head_of_slot.shape[0]
    slot_ids = jnp.arange(slot_total, dtype=jnp.int32)
    return jnp.sum(
        jnp.where(head_of_slot[None, :] == slot_ids[:, None], slot_ids[None, :], 0), axis=1
    )


def greet(axes):
    barrier = pltpu.get_barrier_semaphore()
    total = 0
    for axis in axes:
        n = lax.axis_size(axis)
        me = lax.axis_index(axis)
        for k in range(1, n):
            pl.semaphore_signal(
                barrier, inc=1, device_id={axis: lax.rem(me + k, n)}, device_id_type=MESH
            )
            total += 1
    pl.semaphore_wait(barrier, total)


def remote(src, dst, send_sem, recv_sem, axis, k):
    n = lax.axis_size(axis)
    target = lax.rem(lax.axis_index(axis) + k, n)
    return pltpu.make_async_remote_copy(
        src_ref=src,
        dst_ref=dst,
        send_sem=send_sem,
        recv_sem=recv_sem,
        device_id={axis: target},
        device_id_type=MESH,
    )


def back(axis, index):
    n = lax.axis_size(axis)
    return lax.rem(lax.axis_index(axis) + n - index, n)


def gather_attend_kernel(
    dims, hos, lens, q_ref, kv_hbm, att_ref,
    raw, kv_ref, kv_sem, zq, xs, xr, osend, orecv, lsend, lrecv, scores,
    zq_s, zq_r, xq_s, xq_r, o_s, o_r, l_s, l_r, own_sem,
):
    nc, bq, nsq, hl, ns, per_tp, Lb, hd, G, T = dims
    n_tp, n_seq = lax.axis_size("tp"), lax.axis_size("seq")
    me_t, me_s = lax.axis_index("tp"), lax.axis_index("seq")
    rows = G * T
    block = math.gcd(Lb, 256)
    scale = math.log2(math.e) / math.sqrt(hd)
    fetch = pltpu.make_async_copy(kv_hbm, raw, kv_sem)
    fetch.start()
    greet(("tp", "seq"))

    zsends = [
        [remote(q_ref.at[c], zq[c].at[k], zq_s.at[c, k], zq_r.at[c, k], "tp", k) for k in range(1, n_tp)]
        for c in range(nc)
    ]
    owns = [pltpu.make_async_copy(q_ref.at[c], zq[c].at[0], own_sem.at[c]) for c in range(nc)]
    for c in range(nc):
        for copy in zsends[c]:
            copy.start()
        owns[c].start()

    xsends = [
        [remote(xs.at[c, k], xr.at[c, k], xq_s.at[c, k], xq_r.at[c, k], "seq", k) for k in range(1, n_seq)]
        for c in range(nc)
    ]

    def spread(c):
        owns[c].wait()
        for copy in zsends[c]:
            copy.wait_recv()
        for k in list(range(1, n_seq)) + [0]:
            target = xr if k == 0 else xs
            column = lax.rem(me_s + k, n_seq)
            for j in range(ns):
                head = hos[column * ns + j]
                target[c, k, j] = zq[c][back("tp", head // hl), head % hl]
            if k:
                xsends[c][k - 1].start()

    osends = [
        [remote(osend.at[c, k], orecv.at[c, k], o_s.at[c, k], o_r.at[c, k], "tp", k) for k in range(1, n_tp)]
        for c in range(nc)
    ]
    lsends = [
        [remote(lsend.at[c, k], lrecv.at[c, k], l_s.at[c, k], l_r.at[c, k], "tp", k) for k in range(1, n_tp)]
        for c in range(nc)
    ]

    def attend_pair(c, k, pair):
        x, slot = pair // ns, pair % ns
        plane = lax.rem(me_t + k, n_tp)
        local_seq = plane * bq + x
        whole_seq = plane * per_tp + c * bq + x
        source = back("seq", local_seq // nsq)
        queries = xr[c, source, slot, local_seq % nsq].reshape(rows, hd)
        visible_end = lens[whole_seq] - me_t * Lb
        limits = visible_end - T + lax.broadcasted_iota(jnp.int32, (1, rows), 1) % T
        top = jnp.full((1, rows), FLOOR, jnp.float32)
        for i in range(Lb // block):
            s = lax.dot_general(
                kv_ref[slot, whole_seq, i * block : (i + 1) * block, :hd],
                queries,
                (((1,), (1,)), ((), ())),
                preferred_element_type=jnp.float32,
            )
            pos = i * block + lax.broadcasted_iota(jnp.int32, (block, 1), 0)
            s = jnp.where(pos <= limits, s * scale, MASKED_SCORE)
            scores[i * block : (i + 1) * block, :] = s
            top = jnp.maximum(top, jnp.max(s, axis=0, keepdims=True))
        total = jnp.zeros((1, rows), jnp.float32)
        out = jnp.zeros((hd, rows), jnp.float32)
        for i in range(Lb // block):
            w = jnp.exp2(scores[i * block : (i + 1) * block, :] - top)
            total = total + jnp.sum(w, axis=0, keepdims=True)
            out = out + lax.dot_general(
                kv_ref[slot, whole_seq, i * block : (i + 1) * block, hd:],
                w.astype(jnp.bfloat16),
                (((0,), (0,)), ((), ())),
                preferred_element_type=jnp.float32,
            )
        total = jnp.maximum(total, 1e-30)
        o_to, l_to = (orecv, lrecv) if k == 0 else (osend, lsend)
        o_to[c, k, x, slot] = (out / total).astype(jnp.bfloat16)
        l_to[c, k, x, slot] = top + jnp.log2(total)

    def attend(c):
        for copy in xsends[c]:
            copy.wait_recv()
        order = sorted(range(1, n_tp), key=lambda k: abs(k - n_tp / 2)) + [0]
        for k in order:
            lax.fori_loop(0, bq * ns, lambda pair, _: (attend_pair(c, k, pair), 0)[1], 0)
            if k:
                osends[c][k - 1].start()
                lsends[c][k - 1].start()

    def merge(c):
        for k in range(n_tp - 1):
            osends[c][k].wait_recv()
            lsends[c][k].wait_recv()

        def one(pair, _):
            x, slot = pair // ns, pair % ns
            ls = [lrecv[c, k, x, slot] for k in range(n_tp)]
            top = functools.reduce(jnp.maximum, ls)
            ws = [jnp.exp2(l - top) for l in ls]
            inverse = 1.0 / sum(ws)
            out = jnp.zeros((hd, rows), jnp.float32)
            for k in range(n_tp):
                out = out + (ws[k] * inverse) * orecv[c, k, x, slot].astype(jnp.float32)
            att_ref[c, x, slot] = out.astype(jnp.bfloat16)
            return 0

        lax.fori_loop(0, bq * ns, one, 0)

    fetch.wait()
    step = math.gcd(Lb, 128)
    turns = Lb // step

    def split(turn, _):
        at = pl.ds(pl.multiple_of(turn % turns * step, step), step)
        for slot in range(ns):
            kv_ref[slot, turn // turns, at, :] = raw[turn // turns, at, slot, :]
        return 0

    lax.fori_loop(0, raw.shape[0] * turns, split, 0)
    for c in range(nc):
        spread(c)
        if c:
            attend(c - 1)
    attend(nc - 1)
    for c in range(nc):
        merge(c)
    for c in range(nc):
        for copy in zsends[c] + xsends[c] + osends[c] + lsends[c]:
            copy.wait_send()


def gather_attend(qm, kv, head_of_slot, lengths, dims):
    nc, bq, nsq, hl, ns, per_tp, Lb, hd, G, T = dims
    n_tp, n_seq = lax.axis_size("tp"), lax.axis_size("seq")
    rows = G * T
    bf, f32 = jnp.bfloat16, jnp.float32
    dma = pltpu.SemaphoreType.DMA
    vmem = pl.BlockSpec(memory_space=pltpu.VMEM)
    smem = pl.BlockSpec(memory_space=pltpu.SMEM)
    return pl.pallas_call(
        functools.partial(gather_attend_kernel, dims),
        out_shape=jax.ShapeDtypeStruct((nc, bq, ns, hd, rows), bf),
        in_specs=[smem, smem, vmem, pl.BlockSpec(memory_space=pl.ANY)],
        out_specs=vmem,
        scratch_shapes=[
            pltpu.VMEM(kv.shape, bf),
            pltpu.VMEM((ns, kv.shape[0], Lb, 2 * hd), bf),
            dma(()),
            [pltpu.VMEM((n_tp, hl, nsq, G, T, hd), bf)] * nc,
            pltpu.VMEM((nc, n_seq, ns, nsq, G, T, hd), bf),
            pltpu.VMEM((nc, n_seq, ns, nsq, G, T, hd), bf),
            pltpu.VMEM((nc, n_tp, bq, ns, hd, rows), bf),
            pltpu.VMEM((nc, n_tp, bq, ns, hd, rows), bf),
            pltpu.VMEM((nc, n_tp, bq, ns, 1, rows), f32),
            pltpu.VMEM((nc, n_tp, bq, ns, 1, rows), f32),
            pltpu.VMEM((Lb, rows), f32),
            dma((nc, n_tp)), dma((nc, n_tp)), dma((nc, n_seq)), dma((nc, n_seq)),
            dma((nc, n_tp)), dma((nc, n_tp)), dma((nc, n_tp)), dma((nc, n_tp)), dma((nc,)),
        ],
        compiler_params=pltpu.CompilerParams(
            collective_id=0, has_side_effects=True, vmem_limit_bytes=56 * 2**20
        ),
    )(head_of_slot, lengths, qm, kv)


def project_kernel(
    dims, soh, att_ref, w_hbm, out_ref,
    w_ref, xr, zs, zr, ag, own, ps, pr,
    x_s, x_r, z_s, z_r, a_s, a_r, p_s, p_r, w_sem, own_sem,
):
    nc, bq, hl, ns, sub, part, T = dims
    n_tp, n_seq = lax.axis_size("tp"), lax.axis_size("seq")
    me_t, me_s = lax.axis_index("tp"), lax.axis_index("seq")
    width, columns = w_ref.shape
    few = bq * sub
    load = pltpu.make_async_copy(w_hbm, w_ref, w_sem)
    greet(("tp", "seq"))
    xsends = [
        [
            remote(att_ref.at[c, lax.rem(me_s + k, n_seq)], xr[c].at[k], x_s.at[c, k], x_r.at[c, k], "seq", k)
            for k in range(1, n_seq)
        ]
        for c in range(nc)
    ]
    owns = [pltpu.make_async_copy(att_ref.at[c, me_s], xr[c].at[0], own_sem.at[c]) for c in range(nc)]
    for c in range(nc):
        for copy in xsends[c]:
            copy.start()
        owns[c].start()
    load.start()
    zsends = [
        [remote(zs.at[c, k], zr.at[c, k], z_s.at[c, k], z_r.at[c, k], "tp", k) for k in range(1, n_tp)]
        for c in range(nc)
    ]
    asends = [
        [remote(zr.at[c], ag.at[c, k], a_s.at[c, k], a_r.at[c, k], "seq", k) for k in range(1, n_seq)]
        for c in range(nc)
    ]
    psends = [
        [remote(ps.at[c, k], pr.at[c, k], p_s.at[c, k], p_r.at[c, k], "tp", k) for k in range(1, n_tp)]
        for c in range(nc)
    ]
    for c in range(nc):
        owns[c].wait()
        for copy in xsends[c]:
            copy.wait_recv()
        for k in list(range(1, n_tp)) + [0]:
            target = zr if k == 0 else zs
            plane = lax.rem(me_t + k, n_tp)
            for j in range(hl):
                slot = soh[plane * hl + j]
                picked = xr[c][back("seq", slot // ns), slot % ns]
                target[c, k, :, j * part : (j + 1) * part] = picked
            if k:
                zsends[c][k - 1].start()
    for c in range(nc):
        for copy in zsends[c]:
            copy.wait_recv()
        for copy in asends[c]:
            copy.start()
    load.wait()
    tile = math.gcd(columns, 512)
    for c in range(nc):
        for copy in asends[c]:
            copy.wait_recv()
        pieces = []
        for k in range(n_tp):
            j = (n_tp - k) % n_tp
            for p in range(n_seq):
                pieces.append(zr[c, j] if p == 0 else ag[c, p, j])
        rows = jnp.concatenate(pieces, axis=0)

        def column_tile(i, _):
            at = pl.ds(pl.multiple_of(i * tile, tile), tile)
            product = jnp.dot(rows, w_ref[:, at], preferred_element_type=jnp.float32)
            span = n_seq * few
            own[c, :, at] = product[:span]
            for k in range(1, n_tp):
                ps[c, k, :, at] = product[k * span : (k + 1) * span].astype(jnp.bfloat16)
            return 0

        lax.fori_loop(0, columns // tile, column_tile, 0)
        for copy in psends[c]:
            copy.start()
    for c in range(nc):
        for copy in psends[c]:
            copy.wait_recv()
        for p in range(n_seq):
            column = lax.rem(me_s + n_seq - p, n_seq)
            for x in range(bq):
                at = p * few + x * sub
                total = own[c, at : at + sub]
                for k in range(1, n_tp):
                    total = total + pr[c, k, at : at + sub].astype(jnp.float32)
                out_ref[c * bq + x, pl.ds(pl.multiple_of(column * sub, sub), sub)] = total.astype(jnp.bfloat16)
    for c in range(nc):
        for copy in xsends[c] + zsends[c] + asends[c] + psends[c]:
            copy.wait_send()


def project(att, weight, slot_of_head, dims):
    nc, bq, hl, ns, sub, part, T = dims
    n_tp, n_seq = lax.axis_size("tp"), lax.axis_size("seq")
    width, columns = weight.shape
    few = bq * sub
    bf, f32 = jnp.bfloat16, jnp.float32
    dma = pltpu.SemaphoreType.DMA
    vmem = pl.BlockSpec(memory_space=pltpu.VMEM)
    return pl.pallas_call(
        functools.partial(project_kernel, dims),
        out_shape=jax.ShapeDtypeStruct((nc * bq, T, columns), bf),
        in_specs=[
            pl.BlockSpec(memory_space=pltpu.SMEM), vmem, pl.BlockSpec(memory_space=pl.ANY)
        ],
        out_specs=vmem,
        scratch_shapes=[
            pltpu.VMEM((width, columns), bf),
            [pltpu.VMEM((n_seq, ns, few, part), bf)] * nc,
            pltpu.VMEM((nc, n_tp, few, width), bf),
            pltpu.VMEM((nc, n_tp, few, width), bf),
            pltpu.VMEM((nc, n_seq, n_tp, few, width), bf),
            pltpu.VMEM((nc, n_seq * few, columns), f32),
            pltpu.VMEM((nc, n_tp, n_seq * few, columns), bf),
            pltpu.VMEM((nc, n_tp, n_seq * few, columns), bf),
            dma((nc, n_seq)), dma((nc, n_seq)), dma((nc, n_tp)), dma((nc, n_tp)),
            dma((nc, n_seq)), dma((nc, n_seq)), dma((nc, n_tp)), dma((nc, n_tp)),
            dma(()), dma((nc,)),
        ],
        compiler_params=pltpu.CompilerParams(
            collective_id=1, has_side_effects=True, vmem_limit_bytes=48 * 2**20
        ),
    )(slot_of_head, att, weight)


def line_kernel(
    dims, hos, lens, q_hbm, kv_hbm, w_hbm, out_ref,
    raw, kv_ref, w_ref, az, xs, xr, osend, orecv, lsend, lrecv, scores,
    bs, bls, bm, blm, br, blr, xg, own, ds, dm, dr,
    kv_sem, w_sem, q_sem,
    a_s, a_r, xq_s, xq_r, o_s, o_r, l_s, l_r,
    b_s, b_r, bl_s, bl_r, g_s, g_r, d_s, d_r,
):
    parts, hl, ns, Lb, hd, G = dims
    n_tp, n_seq = lax.axis_size("tp"), lax.axis_size("seq")
    me_t, me_s = lax.axis_index("tp"), lax.axis_index("seq")
    per_tp = out_ref.shape[0]
    nc = len(parts)
    T = out_ref.shape[1]
    columns = w_ref.shape[1]
    half = me_t // 2
    partner = me_t + 1 - 2 * (me_t % 2)
    far_inner = 2 - half
    far_outer = 3 - 3 * half
    inner = me_t == 1 + half
    outer = me_t == 3 * half
    block = math.gcd(Lb, 256)
    scale = math.log2(math.e) / math.sqrt(hd)
    bf, f32 = jnp.bfloat16, jnp.float32

    def to(axis, target, src, dst, send, recv):
        return pltpu.make_async_remote_copy(
            src_ref=src, dst_ref=dst, send_sem=send, recv_sem=recv,
            device_id={axis: target}, device_id_type=MESH,
        )

    def ring(target_of):
        return [[target_of(c, k) for k in range(1, n_seq)] for c in range(nc)]

    def block_to(c, i, plane, target):
        return to("tp", target, az[c].at[plane], az[c].at[plane], a_s.at[c, i], a_r.at[c, i])

    own_p = [block_to(c, 0, me_t, partner) for c in range(nc)]
    own_f = [block_to(c, 1, me_t, far_inner) for c in range(nc)]
    via_f = [block_to(c, 2, partner, far_inner) for c in range(nc)]
    via_a = [block_to(c, 3, far_inner, partner) for c in range(nc)]
    via_b = [block_to(c, 4, far_outer, partner) for c in range(nc)]
    column = lambda k: lax.rem(me_s + k, n_seq)
    xsends = ring(lambda c, k: to("seq", column(k), xs[c].at[k], xr[c].at[k], xq_s.at[c, k], xq_r.at[c, k]))
    osends = ring(lambda c, k: to("seq", column(k), osend[c].at[k], orecv[c].at[k], o_s.at[c, k], o_r.at[c, k]))
    lsends = ring(lambda c, k: to("seq", column(k), lsend[c].at[k], lrecv[c].at[k], l_s.at[c, k], l_r.at[c, k]))
    gsends = ring(lambda c, k: to("seq", column(k), xg[c].at[0], xg[c].at[k], g_s.at[c, k], g_r.at[c, k]))

    def swap(c, send, mid, out, s, r):
        return dict(
            pair=to("tp", partner, send[c].at[0], out[c].at[0], s.at[c, 0], r.at[c, 0]),
            lift=[to("tp", partner, send[c].at[i], mid[c].at[i - 1], s.at[c, i], r.at[c, i]) for i in (1, 2)],
            cross=[
                to("tp", target, send[c].at[i], out[c].at[1], s.at[c, 2 + i], r.at[c, 3])
                for i, target in ((1, far_inner), (2, far_outer))
            ],
        )

    bz = [(swap(c, bs, bm, br, b_s, b_r), swap(c, bls, blm, blr, bl_s, bl_r)) for c in range(nc)]
    dz = [(swap(c, ds, dm, dr, d_s, d_r),) for c in range(nc)]

    def own_blocks(c):
        x, t0, tt = parts[c]
        for j in range(hl):
            for g in range(G):
                yield pltpu.make_async_copy(
                    q_hbm.at[me_s * per_tp + x, pl.ds(t0, tt), pl.ds((j * G + g) * hd, hd)],
                    az[c].at[me_t, j, g],
                    q_sem.at[c],
                )

    def ask_own(c):
        pltpu.make_async_copy(az[c].at[me_t], az[c].at[me_t], q_sem.at[c]).wait()
        own_p[c].start()

        @pl.when(inner)
        def _():
            own_f[c].start()

    def relay_a(c):
        @pl.when(inner)
        def _():
            own_p[c].wait_recv()
            via_f[c].start()
            own_f[c].wait_recv()
            via_a[c].start()

    def relay_b(c):
        @pl.when(inner)
        def _():
            via_f[c].wait_recv()
            via_b[c].start()

    def spread(c):
        @pl.when(outer)
        def _():
            own_p[c].wait_recv()
            via_a[c].wait_recv()
            via_b[c].wait_recv()

        for k in list(range(1, n_seq)) + [0]:
            target = xr if k == 0 else xs
            for j in range(ns):
                head = hos[column(k) * ns + j]
                target[c][k, j] = az[c][head // hl, head % hl]
            if k:
                xsends[c][k - 1].start()

    def attend_pair(c, k, slot):
        x, t0, tt = parts[c]
        rows = G * tt
        seq = column(k) * per_tp + x
        queries = xr[c][(n_seq - k) % n_seq, slot].reshape(rows, hd)
        visible_end = lens[seq] - me_t * Lb
        limits = visible_end - T + t0 + lax.broadcasted_iota(jnp.int32, (1, rows), 1) % tt
        top = jnp.full((1, rows), FLOOR, f32)
        for i in range(Lb // block):
            s = lax.dot_general(
                kv_ref[slot, seq, i * block : (i + 1) * block, :hd],
                queries,
                (((1,), (1,)), ((), ())),
                preferred_element_type=f32,
            )
            pos = i * block + lax.broadcasted_iota(jnp.int32, (block, 1), 0)
            s = jnp.where(pos <= limits, s * scale, MASKED_SCORE)
            scores[i * block : (i + 1) * block, :rows] = s
            top = jnp.maximum(top, jnp.max(s, axis=0, keepdims=True))
        total = jnp.zeros((1, rows), f32)
        out = jnp.zeros((hd, rows), f32)
        for i in range(Lb // block):
            w = jnp.exp2(scores[i * block : (i + 1) * block, :rows] - top)
            total = total + jnp.sum(w, axis=0, keepdims=True)
            out = out + lax.dot_general(
                kv_ref[slot, seq, i * block : (i + 1) * block, hd:],
                w.astype(bf),
                (((0,), (0,)), ((), ())),
                preferred_element_type=f32,
            )
        total = jnp.maximum(total, 1e-30)
        o_to = orecv[c].at[0] if k == 0 else osend[c].at[k]
        l_to = lrecv[c].at[0] if k == 0 else lsend[c].at[k]
        o_to[slot] = (out / total).astype(bf)
        l_to[slot] = top + jnp.log2(total)

    def attend(c, k):
        if k:
            xsends[c][n_seq - k - 1].wait_recv()
        lax.fori_loop(0, ns, lambda slot, _: (attend_pair(c, k, slot), 0)[1], 0)
        if k:
            osends[c][k - 1].start()
            lsends[c][k - 1].start()

    def picked(c, plane, j):
        head = plane * hl + j
        slot = jnp.int32(0)
        for s in range(n_seq * ns):
            slot = jnp.maximum(slot, jnp.where(hos[s] == head, s, 0))
        k = lax.rem(me_s + n_seq - slot // ns, n_seq)
        return orecv[c][k, slot % ns], lrecv[c][k, slot % ns]

    def merged(parts):
        top = functools.reduce(jnp.maximum, [l for _, l in parts])
        ws = [jnp.exp2(l - top) for _, l in parts]
        total = functools.reduce(jnp.add, ws)
        inverse = 1.0 / total
        out = functools.reduce(
            jnp.add, [(w * inverse) * o.astype(f32) for w, (o, _) in zip(ws, parts)]
        )
        return out, top + jnp.log2(total)

    def put(c, i, plane):
        for j in range(hl):
            o, l = picked(c, plane, j)
            bs[c][i, j] = o
            bls[c][i, j] = l

    def part_send(c):
        for copy in osends[c] + lsends[c]:
            copy.wait_recv()

        @pl.when(outer)
        def _():
            for i, plane in ((1, far_inner), (2, far_outer)):
                put(c, i, plane)
                for z in bz[c]:
                    z["lift"][i - 1].start()

        put(c, 0, partner)
        for z in bz[c]:
            z["pair"].start()

    def part_join(c):
        @pl.when(inner)
        def _():
            for i, plane in ((2, far_outer), (1, far_inner)):
                for z in bz[c]:
                    z["lift"][i - 1].wait_recv()
                for j in range(hl):
                    o, l = merged([picked(c, plane, j), (bm[c][i - 1, j], blm[c][i - 1, j])])
                    bs[c][i, j] = o.astype(bf)
                    bls[c][i, j] = l
                for z in bz[c]:
                    z["cross"][i - 1].start()

    def part_end(c):
        tt = parts[c][2]
        for z in bz[c]:
            z["pair"].wait_recv()
            z["cross"][0].wait_recv()
        for j in range(hl):
            o, _ = merged([picked(c, me_t, j)] + [(br[c][i, j], blr[c][i, j]) for i in range(2)])
            turned = o.T.astype(bf)
            for g in range(G):
                at = (j * G + g) * hd
                xg[c][0, :, at : at + hd] = turned[g * tt : (g + 1) * tt]
        for copy in gsends[c]:
            copy.start()

    tile = math.gcd(columns, 512)

    def project(c):
        tt = parts[c][2]
        for copy in gsends[c]:
            copy.wait_recv()
        planes = [me_t, partner, far_inner, far_outer]
        lhs = jnp.concatenate(
            [xg[c][lax.rem(me_s + n_seq - p, n_seq)] for p in planes], axis=0
        )

        def column_tile(i, _):
            at = pl.ds(pl.multiple_of(i * tile, tile), tile)
            product = jnp.dot(lhs, w_ref[:, at], preferred_element_type=f32)
            own[c][:, at] = product[:tt]
            for i in range(3):
                ds[c][i, :, at] = product[(i + 1) * tt : (i + 2) * tt].astype(bf)
            return 0

        lax.fori_loop(0, columns // tile, column_tile, 0)

        @pl.when(outer)
        def _():
            for copy in dz[c][0]["lift"]:
                copy.start()

        dz[c][0]["pair"].start()

    def sum_join(c):
        z = dz[c][0]

        @pl.when(inner)
        def _():
            for i in (2, 1):
                z["lift"][i - 1].wait_recv()
                ds[c][i] = (ds[c][i].astype(f32) + dm[c][i - 1].astype(f32)).astype(bf)
                z["cross"][i - 1].start()

    def sum_end(c):
        x, t0, tt = parts[c]
        z = dz[c][0]
        z["pair"].wait_recv()
        z["cross"][0].wait_recv()
        total = own[c][...] + dr[c][0].astype(f32) + dr[c][1].astype(f32)
        out_ref[x, t0 : t0 + tt] = total.astype(bf)

    step = math.gcd(Lb, 128)
    turns = Lb // step
    n_b = raw.shape[0]
    seq_order = [p * per_tp + x for x in range(per_tp) for p in range(n_tp)]
    fetches = [pltpu.make_async_copy(kv_hbm.at[b], raw.at[b], kv_sem.at[b]) for b in range(n_b)]

    def split(index):
        b = seq_order[index]
        fetches[b].wait()

        def turn(i, _):
            at = pl.ds(pl.multiple_of(i * step, step), step)
            for slot in range(ns):
                kv_ref[slot, b, at, :] = raw[b, at, slot, :]
            return 0

        lax.fori_loop(0, turns, turn, 0)

    load = pltpu.make_async_copy(w_hbm, w_ref, w_sem)

    for c in range(nc):
        for copy in own_blocks(c):
            copy.start()
    for b in seq_order:
        fetches[b].start()
    load.start()
    greet(("tp", "seq"))

    run = dict(
        q=ask_own, ra=relay_a, rb=relay_b, sp=spread, bs=part_send, bj=part_join, be=part_end,
        pr=project, dj=sum_join, de=sum_end, kv=split,
        a0=lambda c: attend(c, 0), a1=lambda c: attend(c, 1),
        a2=lambda c: attend(c, 2), a3=lambda c: attend(c, 3),
    )
    for entry in ORDER:
        name, c = entry.rsplit(".", 1)
        if entry == FIRST_PROJECT:
            load.wait()
        run[name](int(c))

    for c in range(nc):
        own_p[c].wait_send()
        for copy in xsends[c] + osends[c] + lsends[c] + gsends[c]:
            copy.wait_send()
        for z in bz[c] + dz[c]:
            z["pair"].wait_send()

        @pl.when(outer)
        def _():
            for z in bz[c] + dz[c]:
                for copy in z["lift"]:
                    copy.wait_send()

        @pl.when(inner)
        def _():
            for copy in (own_f[c], via_f[c], via_a[c], via_b[c]):
                copy.wait_send()
            for z in bz[c] + dz[c]:
                for copy in z["cross"]:
                    copy.wait_send()


def line_call(query, cache, head_of_slot, lengths, out_weight, cuts):
    n_seq, n_tp = lax.axis_size("seq"), lax.axis_size("tp")
    G = HQ // KVH
    B, T, _ = query.shape
    Lb, ns, hd2 = cache.shape[1:]
    hd = hd2 // 2
    hl = KVH // n_tp
    per_tp = B // n_tp
    parts = []
    for x in range(per_tp):
        t0 = 0
        for tt in cuts[x % len(cuts)]:
            parts.append((x, t0, tt))
            t0 += tt
    sizes = [tt for _, _, tt in parts]
    nc = len(parts)
    columns = out_weight.shape[1]
    bf, f32 = jnp.bfloat16, jnp.float32
    dma = pltpu.SemaphoreType.DMA
    v = pltpu.VMEM
    anywhere = pl.BlockSpec(memory_space=pl.ANY)
    smem = pl.BlockSpec(memory_space=pltpu.SMEM)
    return pl.pallas_call(
        functools.partial(line_kernel, (tuple(parts), hl, ns, Lb, hd, G)),
        out_shape=jax.ShapeDtypeStruct((per_tp, T, columns), bf),
        in_specs=[smem, smem, anywhere, anywhere, anywhere],
        out_specs=pl.BlockSpec(memory_space=pltpu.VMEM),
        scratch_shapes=[
            v(cache.shape, bf),
            v((ns, B, Lb, 2 * hd), bf),
            v(out_weight.shape, bf),
            [v((n_tp, hl, G, tt, hd), bf) for tt in sizes],
            [v((n_seq, ns, G, tt, hd), bf) for tt in sizes],
            [v((n_seq, ns, G, tt, hd), bf) for tt in sizes],
            [v((n_seq, ns, hd, G * tt), bf) for tt in sizes],
            [v((n_seq, ns, hd, G * tt), bf) for tt in sizes],
            [v((n_seq, ns, 1, G * tt), f32) for tt in sizes],
            [v((n_seq, ns, 1, G * tt), f32) for tt in sizes],
            v((Lb, G * max(sizes)), f32),
            [v((3, hl, hd, G * tt), bf) for tt in sizes], [v((3, hl, 1, G * tt), f32) for tt in sizes],
            [v((2, hl, hd, G * tt), bf) for tt in sizes], [v((2, hl, 1, G * tt), f32) for tt in sizes],
            [v((2, hl, hd, G * tt), bf) for tt in sizes], [v((2, hl, 1, G * tt), f32) for tt in sizes],
            [v((n_seq, tt, hl * G * hd), bf) for tt in sizes],
            [v((tt, columns), f32) for tt in sizes],
            [v((3, tt, columns), bf) for tt in sizes],
            [v((2, tt, columns), bf) for tt in sizes],
            [v((2, tt, columns), bf) for tt in sizes],
            dma((B,)), dma(()), dma((nc,)),
            dma((nc, 5)), dma((nc, 5)),
            dma((nc, n_seq)), dma((nc, n_seq)),
            dma((nc, n_seq)), dma((nc, n_seq)), dma((nc, n_seq)), dma((nc, n_seq)),
            dma((nc, 5)), dma((nc, 4)), dma((nc, 5)), dma((nc, 4)),
            dma((nc, n_seq)), dma((nc, n_seq)),
            dma((nc, 5)), dma((nc, 4)),
        ],
        compiler_params=pltpu.CompilerParams(
            collective_id=2, has_side_effects=True, vmem_limit_bytes=60 * 2**20
        ),
    )(head_of_slot, lengths, query, cache, out_weight)


def local(query, cache, head_of_slot, lengths, out_weight):
    G = HQ // KVH
    n_seq, n_tp = lax.axis_size("seq"), lax.axis_size("tp")
    me_s = lax.axis_index("seq")
    slot_of_head = slot_table(head_of_slot)
    B, T, width = query.shape
    Lb, ns, hd2 = cache.shape[1:]
    hd = hd2 // 2
    hl = KVH // n_tp
    per_tp = B // n_tp
    fits = all(sum(cut) == T for cut in CUTS) and len(CUTS) == per_tp
    if n_tp == n_seq == 4 and HQ * hd == n_tp * width and fits:
        return line_call(query, cache, head_of_slot, lengths, out_weight, CUTS)
    nc = math.gcd(CHUNKS, per_tp)
    bq = per_tp // nc
    nsq = n_tp * bq // n_seq
    sub = T // n_seq

    chunked = query.reshape(n_tp, nc, bq, T, width).transpose(1, 0, 2, 3, 4)
    chunked = chunked.reshape(nc, n_seq, nsq, T, width)
    mine = lax.dynamic_index_in_dim(chunked, me_s, 1, False)
    qm = mine.reshape(nc, nsq, T, hl, G, hd).transpose(0, 3, 1, 4, 2, 5)
    kv = cache
    att = gather_attend(
        qm, kv, head_of_slot, lengths, (nc, bq, nsq, hl, ns, per_tp, Lb, hd, G, T)
    )
    att = att.reshape(nc, bq, ns, hd, G, n_seq, sub).transpose(0, 5, 2, 1, 6, 4, 3)
    att = att.reshape(nc, n_seq, ns, bq * sub, G * hd)
    return project(att, out_weight, slot_of_head, (nc, bq, hl, ns, sub, G * hd, T))


def solution(mesh):
    in_specs = (
        P("grp", None, "tp"),
        P("grp", "tp", "seq", None),
        P("grp"),
        P("grp"),
        P("tp", "seq"),
    )
    out_specs = P(("grp", "tp"), None, "seq")
    return jax.shard_map(local, mesh=mesh, in_specs=in_specs, out_specs=out_specs, check_vma=False)
```

```python
import functools
import math

import jax
import jax.numpy as jnp
from jax import lax
from jax.experimental import pallas as pl
from jax.experimental.pallas import tpu as pltpu
from jax.sharding import PartitionSpec as P

HQ = 64
KVH = 8
CHUNKS = 2
SLOTS = 3
CUTS = ((16, 16, 16, 16), (16, 32, 16))
ORDER = (
    "kv.0", "hello.0", "q.0", "q.1", "kv.1", "kv.2", "ra.0", "ra.1", "kv.3", "rb.0", "kv.4",
    "rb.1", "q.2", "kv.5", "q.3", "kv.6", "sp.0", "kv.7", "ra.2", "ra.3", "sp.1", "a0.0", "a1.0",
    "rb.2", "q.4", "a2.0", "a0.1", "rb.3", "ra.4", "a3.0", "a1.1", "q.5", "sp.2", "a0.2", "a2.1",
    "a3.1", "bs.0", "rb.4", "sp.3", "kv.8", "kv.9", "a1.2", "ra.5", "a2.2", "bj.0", "a3.2",
    "bs.1", "q.6", "a0.3", "a1.3", "a2.3", "bj.1", "a3.3", "kv.10", "rb.5", "sp.4", "kv.11",
    "kv.12", "be.0", "bs.2", "bs.3", "kv.13", "kv.14", "be.1", "kv.15", "a0.4", "bj.2", "sp.5",
    "ra.6", "a1.4", "pr.0", "bj.3", "pr.1", "a2.4", "a3.4", "a0.5", "be.2", "a1.5", "dj.0",
    "a2.5", "rb.6", "dj.1", "bs.4", "a3.5", "pr.2", "sp.6", "be.3", "bj.4", "bs.5", "a0.6",
    "a1.6", "a2.6", "a3.6", "bj.5", "dj.2", "pr.3", "be.4", "dj.3", "be.5", "bs.6", "bj.6",
    "pr.4", "dj.4", "de.3", "pr.5", "be.6", "de.2", "dj.5", "de.0", "pr.6", "de.4", "de.1",
    "dj.6", "de.5", "de.6",
)
FIRST_PROJECT = next(e for e in ORDER if e[:2] == "pr")
MASKED_SCORE = -1e30
FLOOR = -1e29
MESH = pl.DeviceIdType.MESH


def slot_table(head_of_slot):
    slot_total = head_of_slot.shape[0]
    slot_ids = jnp.arange(slot_total, dtype=jnp.int32)
    return jnp.sum(
        jnp.where(head_of_slot[None, :] == slot_ids[:, None], slot_ids[None, :], 0), axis=1
    )


def greet(axes):
    barrier = pltpu.get_barrier_semaphore()
    total = 0
    for axis in axes:
        n = lax.axis_size(axis)
        me = lax.axis_index(axis)
        for k in range(1, n):
            pl.semaphore_signal(
                barrier, inc=1, device_id={axis: lax.rem(me + k, n)}, device_id_type=MESH
            )
            total += 1
    pl.semaphore_wait(barrier, total)


def remote(src, dst, send_sem, recv_sem, axis, k):
    n = lax.axis_size(axis)
    target = lax.rem(lax.axis_index(axis) + k, n)
    return pltpu.make_async_remote_copy(
        src_ref=src,
        dst_ref=dst,
        send_sem=send_sem,
        recv_sem=recv_sem,
        device_id={axis: target},
        device_id_type=MESH,
    )


def back(axis, index):
    n = lax.axis_size(axis)
    return lax.rem(lax.axis_index(axis) + n - index, n)


def gather_attend_kernel(
    dims, hos, lens, q_ref, kv_hbm, att_ref,
    raw, kv_ref, kv_sem, zq, xs, xr, osend, orecv, lsend, lrecv, scores,
    zq_s, zq_r, xq_s, xq_r, o_s, o_r, l_s, l_r, own_sem,
):
    nc, bq, nsq, hl, ns, per_tp, Lb, hd, G, T = dims
    n_tp, n_seq = lax.axis_size("tp"), lax.axis_size("seq")
    me_t, me_s = lax.axis_index("tp"), lax.axis_index("seq")
    rows = G * T
    block = math.gcd(Lb, 256)
    scale = math.log2(math.e) / math.sqrt(hd)
    fetch = pltpu.make_async_copy(kv_hbm, raw, kv_sem)
    fetch.start()
    greet(("tp", "seq"))

    zsends = [
        [remote(q_ref.at[c], zq[c].at[k], zq_s.at[c, k], zq_r.at[c, k], "tp", k) for k in range(1, n_tp)]
        for c in range(nc)
    ]
    owns = [pltpu.make_async_copy(q_ref.at[c], zq[c].at[0], own_sem.at[c]) for c in range(nc)]
    for c in range(nc):
        for copy in zsends[c]:
            copy.start()
        owns[c].start()

    xsends = [
        [remote(xs.at[c, k], xr.at[c, k], xq_s.at[c, k], xq_r.at[c, k], "seq", k) for k in range(1, n_seq)]
        for c in range(nc)
    ]

    def spread(c):
        owns[c].wait()
        for copy in zsends[c]:
            copy.wait_recv()
        for k in list(range(1, n_seq)) + [0]:
            target = xr if k == 0 else xs
            column = lax.rem(me_s + k, n_seq)
            for j in range(ns):
                head = hos[column * ns + j]
                target[c, k, j] = zq[c][back("tp", head // hl), head % hl]
            if k:
                xsends[c][k - 1].start()

    osends = [
        [remote(osend.at[c, k], orecv.at[c, k], o_s.at[c, k], o_r.at[c, k], "tp", k) for k in range(1, n_tp)]
        for c in range(nc)
    ]
    lsends = [
        [remote(lsend.at[c, k], lrecv.at[c, k], l_s.at[c, k], l_r.at[c, k], "tp", k) for k in range(1, n_tp)]
        for c in range(nc)
    ]

    def attend_pair(c, k, pair):
        x, slot = pair // ns, pair % ns
        plane = lax.rem(me_t + k, n_tp)
        local_seq = plane * bq + x
        whole_seq = plane * per_tp + c * bq + x
        source = back("seq", local_seq // nsq)
        queries = xr[c, source, slot, local_seq % nsq].reshape(rows, hd)
        visible_end = lens[whole_seq] - me_t * Lb
        limits = visible_end - T + lax.broadcasted_iota(jnp.int32, (1, rows), 1) % T
        top = jnp.full((1, rows), FLOOR, jnp.float32)
        for i in range(Lb // block):
            s = lax.dot_general(
                kv_ref[slot, whole_seq, i * block : (i + 1) * block, :hd],
                queries,
                (((1,), (1,)), ((), ())),
                preferred_element_type=jnp.float32,
            )
            pos = i * block + lax.broadcasted_iota(jnp.int32, (block, 1), 0)
            s = jnp.where(pos <= limits, s * scale, MASKED_SCORE)
            scores[i * block : (i + 1) * block, :] = s
            top = jnp.maximum(top, jnp.max(s, axis=0, keepdims=True))
        total = jnp.zeros((1, rows), jnp.float32)
        out = jnp.zeros((hd, rows), jnp.float32)
        for i in range(Lb // block):
            w = jnp.exp2(scores[i * block : (i + 1) * block, :] - top)
            total = total + jnp.sum(w, axis=0, keepdims=True)
            out = out + lax.dot_general(
                kv_ref[slot, whole_seq, i * block : (i + 1) * block, hd:],
                w.astype(jnp.bfloat16),
                (((0,), (0,)), ((), ())),
                preferred_element_type=jnp.float32,
            )
        total = jnp.maximum(total, 1e-30)
        o_to, l_to = (orecv, lrecv) if k == 0 else (osend, lsend)
        o_to[c, k, x, slot] = (out / total).astype(jnp.bfloat16)
        l_to[c, k, x, slot] = top + jnp.log2(total)

    def attend(c):
        for copy in xsends[c]:
            copy.wait_recv()
        order = sorted(range(1, n_tp), key=lambda k: abs(k - n_tp / 2)) + [0]
        for k in order:
            lax.fori_loop(0, bq * ns, lambda pair, _: (attend_pair(c, k, pair), 0)[1], 0)
            if k:
                osends[c][k - 1].start()
                lsends[c][k - 1].start()

    def merge(c):
        for k in range(n_tp - 1):
            osends[c][k].wait_recv()
            lsends[c][k].wait_recv()

        def one(pair, _):
            x, slot = pair // ns, pair % ns
            ls = [lrecv[c, k, x, slot] for k in range(n_tp)]
            top = functools.reduce(jnp.maximum, ls)
            ws = [jnp.exp2(l - top) for l in ls]
            inverse = 1.0 / sum(ws)
            out = jnp.zeros((hd, rows), jnp.float32)
            for k in range(n_tp):
                out = out + (ws[k] * inverse) * orecv[c, k, x, slot].astype(jnp.float32)
            att_ref[c, x, slot] = out.astype(jnp.bfloat16)
            return 0

        lax.fori_loop(0, bq * ns, one, 0)

    fetch.wait()
    step = math.gcd(Lb, 128)
    turns = Lb // step

    def split(turn, _):
        at = pl.ds(pl.multiple_of(turn % turns * step, step), step)
        for slot in range(ns):
            kv_ref[slot, turn // turns, at, :] = raw[turn // turns, at, slot, :]
        return 0

    lax.fori_loop(0, raw.shape[0] * turns, split, 0)
    for c in range(nc):
        spread(c)
        if c:
            attend(c - 1)
    attend(nc - 1)
    for c in range(nc):
        merge(c)
    for c in range(nc):
        for copy in zsends[c] + xsends[c] + osends[c] + lsends[c]:
            copy.wait_send()


def gather_attend(qm, kv, head_of_slot, lengths, dims):
    nc, bq, nsq, hl, ns, per_tp, Lb, hd, G, T = dims
    n_tp, n_seq = lax.axis_size("tp"), lax.axis_size("seq")
    rows = G * T
    bf, f32 = jnp.bfloat16, jnp.float32
    dma = pltpu.SemaphoreType.DMA
    vmem = pl.BlockSpec(memory_space=pltpu.VMEM)
    smem = pl.BlockSpec(memory_space=pltpu.SMEM)
    return pl.pallas_call(
        functools.partial(gather_attend_kernel, dims),
        out_shape=jax.ShapeDtypeStruct((nc, bq, ns, hd, rows), bf),
        in_specs=[smem, smem, vmem, pl.BlockSpec(memory_space=pl.ANY)],
        out_specs=vmem,
        scratch_shapes=[
            pltpu.VMEM(kv.shape, bf),
            pltpu.VMEM((ns, kv.shape[0], Lb, 2 * hd), bf),
            dma(()),
            [pltpu.VMEM((n_tp, hl, nsq, G, T, hd), bf)] * nc,
            pltpu.VMEM((nc, n_seq, ns, nsq, G, T, hd), bf),
            pltpu.VMEM((nc, n_seq, ns, nsq, G, T, hd), bf),
            pltpu.VMEM((nc, n_tp, bq, ns, hd, rows), bf),
            pltpu.VMEM((nc, n_tp, bq, ns, hd, rows), bf),
            pltpu.VMEM((nc, n_tp, bq, ns, 1, rows), f32),
            pltpu.VMEM((nc, n_tp, bq, ns, 1, rows), f32),
            pltpu.VMEM((Lb, rows), f32),
            dma((nc, n_tp)), dma((nc, n_tp)), dma((nc, n_seq)), dma((nc, n_seq)),
            dma((nc, n_tp)), dma((nc, n_tp)), dma((nc, n_tp)), dma((nc, n_tp)), dma((nc,)),
        ],
        compiler_params=pltpu.CompilerParams(
            collective_id=0, has_side_effects=True, vmem_limit_bytes=56 * 2**20
        ),
    )(head_of_slot, lengths, qm, kv)


def project_kernel(
    dims, soh, att_ref, w_hbm, out_ref,
    w_ref, xr, zs, zr, ag, own, ps, pr,
    x_s, x_r, z_s, z_r, a_s, a_r, p_s, p_r, w_sem, own_sem,
):
    nc, bq, hl, ns, sub, part, T = dims
    n_tp, n_seq = lax.axis_size("tp"), lax.axis_size("seq")
    me_t, me_s = lax.axis_index("tp"), lax.axis_index("seq")
    width, columns = w_ref.shape
    few = bq * sub
    load = pltpu.make_async_copy(w_hbm, w_ref, w_sem)
    greet(("tp", "seq"))
    xsends = [
        [
            remote(att_ref.at[c, lax.rem(me_s + k, n_seq)], xr[c].at[k], x_s.at[c, k], x_r.at[c, k], "seq", k)
            for k in range(1, n_seq)
        ]
        for c in range(nc)
    ]
    owns = [pltpu.make_async_copy(att_ref.at[c, me_s], xr[c].at[0], own_sem.at[c]) for c in range(nc)]
    for c in range(nc):
        for copy in xsends[c]:
            copy.start()
        owns[c].start()
    load.start()
    zsends = [
        [remote(zs.at[c, k], zr.at[c, k], z_s.at[c, k], z_r.at[c, k], "tp", k) for k in range(1, n_tp)]
        for c in range(nc)
    ]
    asends = [
        [remote(zr.at[c], ag.at[c, k], a_s.at[c, k], a_r.at[c, k], "seq", k) for k in range(1, n_seq)]
        for c in range(nc)
    ]
    psends = [
        [remote(ps.at[c, k], pr.at[c, k], p_s.at[c, k], p_r.at[c, k], "tp", k) for k in range(1, n_tp)]
        for c in range(nc)
    ]
    for c in range(nc):
        owns[c].wait()
        for copy in xsends[c]:
            copy.wait_recv()
        for k in list(range(1, n_tp)) + [0]:
            target = zr if k == 0 else zs
            plane = lax.rem(me_t + k, n_tp)
            for j in range(hl):
                slot = soh[plane * hl + j]
                picked = xr[c][back("seq", slot // ns), slot % ns]
                target[c, k, :, j * part : (j + 1) * part] = picked
            if k:
                zsends[c][k - 1].start()
    for c in range(nc):
        for copy in zsends[c]:
            copy.wait_recv()
        for copy in asends[c]:
            copy.start()
    load.wait()
    tile = math.gcd(columns, 512)
    for c in range(nc):
        for copy in asends[c]:
            copy.wait_recv()
        pieces = []
        for k in range(n_tp):
            j = (n_tp - k) % n_tp
            for p in range(n_seq):
                pieces.append(zr[c, j] if p == 0 else ag[c, p, j])
        rows = jnp.concatenate(pieces, axis=0)

        def column_tile(i, _):
            at = pl.ds(pl.multiple_of(i * tile, tile), tile)
            product = jnp.dot(rows, w_ref[:, at], preferred_element_type=jnp.float32)
            span = n_seq * few
            own[c, :, at] = product[:span]
            for k in range(1, n_tp):
                ps[c, k, :, at] = product[k * span : (k + 1) * span].astype(jnp.bfloat16)
            return 0

        lax.fori_loop(0, columns // tile, column_tile, 0)
        for copy in psends[c]:
            copy.start()
    for c in range(nc):
        for copy in psends[c]:
            copy.wait_recv()
        for p in range(n_seq):
            column = lax.rem(me_s + n_seq - p, n_seq)
            for x in range(bq):
                at = p * few + x * sub
                total = own[c, at : at + sub]
                for k in range(1, n_tp):
                    total = total + pr[c, k, at : at + sub].astype(jnp.float32)
                out_ref[c * bq + x, pl.ds(pl.multiple_of(column * sub, sub), sub)] = total.astype(jnp.bfloat16)
    for c in range(nc):
        for copy in xsends[c] + zsends[c] + asends[c] + psends[c]:
            copy.wait_send()


def project(att, weight, slot_of_head, dims):
    nc, bq, hl, ns, sub, part, T = dims
    n_tp, n_seq = lax.axis_size("tp"), lax.axis_size("seq")
    width, columns = weight.shape
    few = bq * sub
    bf, f32 = jnp.bfloat16, jnp.float32
    dma = pltpu.SemaphoreType.DMA
    vmem = pl.BlockSpec(memory_space=pltpu.VMEM)
    return pl.pallas_call(
        functools.partial(project_kernel, dims),
        out_shape=jax.ShapeDtypeStruct((nc * bq, T, columns), bf),
        in_specs=[
            pl.BlockSpec(memory_space=pltpu.SMEM), vmem, pl.BlockSpec(memory_space=pl.ANY)
        ],
        out_specs=vmem,
        scratch_shapes=[
            pltpu.VMEM((width, columns), bf),
            [pltpu.VMEM((n_seq, ns, few, part), bf)] * nc,
            pltpu.VMEM((nc, n_tp, few, width), bf),
            pltpu.VMEM((nc, n_tp, few, width), bf),
            pltpu.VMEM((nc, n_seq, n_tp, few, width), bf),
            pltpu.VMEM((nc, n_seq * few, columns), f32),
            pltpu.VMEM((nc, n_tp, n_seq * few, columns), bf),
            pltpu.VMEM((nc, n_tp, n_seq * few, columns), bf),
            dma((nc, n_seq)), dma((nc, n_seq)), dma((nc, n_tp)), dma((nc, n_tp)),
            dma((nc, n_seq)), dma((nc, n_seq)), dma((nc, n_tp)), dma((nc, n_tp)),
            dma(()), dma((nc,)),
        ],
        compiler_params=pltpu.CompilerParams(
            collective_id=1, has_side_effects=True, vmem_limit_bytes=48 * 2**20
        ),
    )(slot_of_head, att, weight)


def greet_start(axes):
    barrier = pltpu.get_barrier_semaphore()
    total = 0
    for axis in axes:
        n = lax.axis_size(axis)
        me = lax.axis_index(axis)
        for k in range(1, n):
            pl.semaphore_signal(
                barrier, inc=1, device_id={axis: lax.rem(me + k, n)}, device_id_type=MESH
            )
            total += 1
    return total


def line_kernel(
    dims, hos, lens, q_hbm, kv_hbm, w_hbm, out_hbm,
    raw, kv_ref, w_ref, az, xs, xr, osend, orecv, lsend, lrecv, scores,
    bs, bls, bm, blm, br, blr, xg, own, ds, dm, dr,
    kv_sem, w_sem, q_sem,
    a_s, a_r, xq_s, xq_r, o_s, o_r, l_s, l_r,
    b_s, b_r, bl_s, bl_r, g_s, g_r, d_s, d_r, out_ref, out_sem,
):
    parts, hl, ns, Lb, hd, G = dims
    n_tp, n_seq = lax.axis_size("tp"), lax.axis_size("seq")
    me_t, me_s = lax.axis_index("tp"), lax.axis_index("seq")
    per_tp = out_hbm.shape[0]
    nc = len(parts)
    T = out_hbm.shape[1]
    columns = w_ref.shape[1]
    half = me_t // 2
    partner = me_t + 1 - 2 * (me_t % 2)
    far_inner = 2 - half
    far_outer = 3 - 3 * half
    inner = me_t == 1 + half
    outer = me_t == 3 * half
    block = math.gcd(Lb, 256)
    scale = math.log2(math.e) / math.sqrt(hd)
    bf, f32 = jnp.bfloat16, jnp.float32

    def to(axis, target, src, dst, send, recv):
        return pltpu.make_async_remote_copy(
            src_ref=src, dst_ref=dst, send_sem=send, recv_sem=recv,
            device_id={axis: target}, device_id_type=MESH,
        )

    def ring(target_of):
        return {k: [target_of(c, k) for c in range(nc)] for k in range(1, n_seq)}

    turn_of = {}
    for entry in ORDER:
        name, c = entry.rsplit(".", 1)
        turn_of.setdefault(name, []).append(int(c))

    def slot(name, c):
        return turn_of[name].index(c) % SLOTS

    def begin(name, c, copies):
        turn = turn_of[name].index(c)
        if turn >= SLOTS:
            copies[turn_of[name][turn - SLOTS]].wait_send()
        copies[c].start()

    def finish(name, copies):
        for c in turn_of[name][-SLOTS:]:
            copies[c].wait_send()

    def block_to(c, name, i, r, plane, target):
        return to(
            "tp", target, az[c].at[plane], az[c].at[plane], a_s.at[slot(name, c), i], a_r.at[c, r]
        )

    own_p = [block_to(c, "q", 0, 0, me_t, partner) for c in range(nc)]
    own_f = [block_to(c, "q", 1, 1, me_t, far_inner) for c in range(nc)]
    via_f = [block_to(c, "ra", 2, 2, partner, far_inner) for c in range(nc)]
    via_a = [block_to(c, "ra", 3, 1, far_inner, partner) for c in range(nc)]
    via_b = [block_to(c, "rb", 4, 2, far_outer, partner) for c in range(nc)]
    column = lambda k: lax.rem(me_s + k, n_seq)
    xsends = ring(lambda c, k: to("seq", column(k), xs[c].at[k], xr[c].at[k], xq_s.at[slot("sp", c), k - 1], xq_r.at[c, k - 1]))
    osends = ring(lambda c, k: to("seq", column(k), osend[c].at[k], orecv[c].at[k], o_s.at[slot(f"a{k}", c), k - 1], o_r.at[c, k - 1]))
    lsends = ring(lambda c, k: to("seq", column(k), lsend[c].at[k], lrecv[c].at[k], l_s.at[slot(f"a{k}", c), k - 1], l_r.at[c, k - 1]))
    gsends = ring(lambda c, k: to("seq", column(k), xg[c].at[0], xg[c].at[k], g_s.at[slot("be", c), k - 1], g_r.at[c, k - 1]))

    def swap(first, second, send, mid, out, s, r):
        def one(c, name, i, r_i, target, dst):
            return to("tp", target, send[c].at[i], dst, s.at[slot(name, c), i], r.at[c, r_i])

        return dict(
            pair=[one(c, first, 0, 0, partner, out[c].at[0]) for c in range(nc)],
            lift={i: [one(c, first, i, i, partner, mid[c].at[i - 1]) for c in range(nc)] for i in (1, 2)},
            cross={
                i: [
                    to("tp", target, send[c].at[i], out[c].at[1], s.at[slot(second, c), 2 + i], r.at[c, 3])
                    for c in range(nc)
                ]
                for i, target in ((1, far_inner), (2, far_outer))
            },
        )

    bz = (swap("bs", "bj", bs, bm, br, b_s, b_r), swap("bs", "bj", bls, blm, blr, bl_s, bl_r))
    dz = (swap("pr", "dj", ds, dm, dr, d_s, d_r),)

    def own_blocks(c):
        x, t0, tt = parts[c]
        for j in range(hl):
            for g in range(G):
                yield pltpu.make_async_copy(
                    q_hbm.at[me_s * per_tp + x, pl.ds(t0, tt), pl.ds((j * G + g) * hd, hd)],
                    az[c].at[me_t, j, g],
                    q_sem.at[c],
                )

    def ask_own(c):
        pltpu.make_async_copy(az[c].at[me_t], az[c].at[me_t], q_sem.at[c]).wait()
        begin("q", c, own_p)

        @pl.when(inner)
        def _():
            begin("q", c, own_f)

    def relay_a(c):
        @pl.when(inner)
        def _():
            own_p[c].wait_recv()
            begin("ra", c, via_f)
            own_f[c].wait_recv()
            begin("ra", c, via_a)

    def relay_b(c):
        @pl.when(inner)
        def _():
            via_f[c].wait_recv()
            begin("rb", c, via_b)

    def spread(c):
        @pl.when(outer)
        def _():
            own_p[c].wait_recv()
            via_a[c].wait_recv()
            via_b[c].wait_recv()

        for k in list(range(1, n_seq)) + [0]:
            target = xr if k == 0 else xs
            for j in range(ns):
                head = hos[column(k) * ns + j]
                target[c][k, j] = az[c][head // hl, head % hl]
            if k:
                begin("sp", c, xsends[k])

    def attend_pair(c, k, slot):
        x, t0, tt = parts[c]
        rows = G * tt
        seq = column(k) * per_tp + x
        queries = xr[c][(n_seq - k) % n_seq, slot].reshape(rows, hd)
        visible_end = lens[seq] - me_t * Lb
        limits = visible_end - T + t0 + lax.broadcasted_iota(jnp.int32, (1, rows), 1) % tt
        top = jnp.full((1, rows), FLOOR, f32)
        for i in range(Lb // block):
            s = lax.dot_general(
                kv_ref[slot, seq, i * block : (i + 1) * block, :hd],
                queries,
                (((1,), (1,)), ((), ())),
                preferred_element_type=f32,
            )
            pos = i * block + lax.broadcasted_iota(jnp.int32, (block, 1), 0)
            s = jnp.where(pos <= limits, s * scale, MASKED_SCORE)
            scores[i * block : (i + 1) * block, :rows] = s
            top = jnp.maximum(top, jnp.max(s, axis=0, keepdims=True))
        total = jnp.zeros((1, rows), f32)
        out = jnp.zeros((hd, rows), f32)
        for i in range(Lb // block):
            w = jnp.exp2(scores[i * block : (i + 1) * block, :rows] - top)
            total = total + jnp.sum(w, axis=0, keepdims=True)
            out = out + lax.dot_general(
                kv_ref[slot, seq, i * block : (i + 1) * block, hd:],
                w.astype(bf),
                (((0,), (0,)), ((), ())),
                preferred_element_type=f32,
            )
        total = jnp.maximum(total, 1e-30)
        o_to = orecv[c].at[0] if k == 0 else osend[c].at[k]
        l_to = lrecv[c].at[0] if k == 0 else lsend[c].at[k]
        o_to[slot] = (out / total).astype(bf)
        l_to[slot] = top + jnp.log2(total)

    def attend(c, k):
        if k:
            xsends[n_seq - k][c].wait_recv()
        lax.fori_loop(0, ns, lambda slot, _: (attend_pair(c, k, slot), 0)[1], 0)
        if k:
            begin(f"a{k}", c, osends[k])
            begin(f"a{k}", c, lsends[k])

    def picked(c, plane, j):
        head = plane * hl + j
        slot = jnp.int32(0)
        for s in range(n_seq * ns):
            slot = jnp.maximum(slot, jnp.where(hos[s] == head, s, 0))
        k = lax.rem(me_s + n_seq - slot // ns, n_seq)
        return orecv[c][k, slot % ns], lrecv[c][k, slot % ns]

    def merged(parts):
        top = functools.reduce(jnp.maximum, [l for _, l in parts])
        ws = [jnp.exp2(l - top) for _, l in parts]
        total = functools.reduce(jnp.add, ws)
        inverse = 1.0 / total
        out = functools.reduce(
            jnp.add, [(w * inverse) * o.astype(f32) for w, (o, _) in zip(ws, parts)]
        )
        return out, top + jnp.log2(total)

    def put(c, i, plane):
        for j in range(hl):
            o, l = picked(c, plane, j)
            bs[c][i, j] = o
            bls[c][i, j] = l

    def part_send(c):
        for k in range(1, n_seq):
            osends[k][c].wait_recv()
            lsends[k][c].wait_recv()

        @pl.when(outer)
        def _():
            for i, plane in ((2, far_outer), (1, far_inner)):
                put(c, i, plane)
                for z in bz:
                    begin("bs", c, z["lift"][i])

        put(c, 0, partner)
        for z in bz:
            begin("bs", c, z["pair"])

    def part_join(c):
        @pl.when(inner)
        def _():
            for i, plane in ((2, far_outer), (1, far_inner)):
                for z in bz:
                    z["lift"][i][c].wait_recv()
                for j in range(hl):
                    o, l = merged([picked(c, plane, j), (bm[c][i - 1, j], blm[c][i - 1, j])])
                    bs[c][i, j] = o.astype(bf)
                    bls[c][i, j] = l
                for z in bz:
                    begin("bj", c, z["cross"][i])

    def part_end(c):
        tt = parts[c][2]
        for z in bz:
            z["pair"][c].wait_recv()
            z["cross"][1][c].wait_recv()
        for j in range(hl):
            o, _ = merged([picked(c, me_t, j)] + [(br[c][i, j], blr[c][i, j]) for i in range(2)])
            turned = o.T.astype(bf)
            for g in range(G):
                at = (j * G + g) * hd
                xg[c][0, :, at : at + hd] = turned[g * tt : (g + 1) * tt]
        for k in range(1, n_seq):
            begin("be", c, gsends[k])

    tile = math.gcd(columns, 512)

    def project(c):
        tt = parts[c][2]
        for k in range(1, n_seq):
            gsends[k][c].wait_recv()
        planes = [me_t, partner, far_inner, far_outer]
        lhs = jnp.concatenate(
            [xg[c][lax.rem(me_s + n_seq - p, n_seq)] for p in planes], axis=0
        )

        def column_tile(i, _):
            at = pl.ds(pl.multiple_of(i * tile, tile), tile)
            product = jnp.dot(lhs, w_ref[:, at], preferred_element_type=f32)
            own[c][:, at] = product[:tt]
            for i in range(3):
                ds[c][i, :, at] = product[(i + 1) * tt : (i + 2) * tt].astype(bf)
            return 0

        lax.fori_loop(0, columns // tile, column_tile, 0)

        @pl.when(outer)
        def _():
            for i in (2, 1):
                begin("pr", c, dz[0]["lift"][i])

        begin("pr", c, dz[0]["pair"])

    def sum_join(c):
        z = dz[0]

        @pl.when(inner)
        def _():
            for i in (2, 1):
                z["lift"][i][c].wait_recv()
                ds[c][i] = (ds[c][i].astype(f32) + dm[c][i - 1].astype(f32)).astype(bf)
                begin("dj", c, z["cross"][i])

    def sum_end(c):
        x, t0, tt = parts[c]
        z = dz[0]
        z["pair"][c].wait_recv()
        z["cross"][1][c].wait_recv()
        total = own[c][...] + dr[c][0].astype(f32) + dr[c][1].astype(f32)
        out_ref[x, t0 : t0 + tt] = total.astype(bf)
        gives[c].start()

    step = math.gcd(Lb, 128)
    turns = Lb // step
    n_b = raw.shape[0]
    seq_order = [p * per_tp + x for x in range(per_tp) for p in range(n_tp)]
    fetches = [pltpu.make_async_copy(kv_hbm.at[b], raw.at[b], kv_sem.at[b]) for b in range(n_b)]

    def split(index):
        b = seq_order[index // 2]
        if index % 2 == 0:
            fetches[b].wait()
        first = index % 2 * (turns // 2)
        last = turns if index % 2 else turns // 2

        def turn(i, _):
            at = pl.ds(pl.multiple_of(i * step, step), step)
            for slot in range(ns):
                kv_ref[slot, b, at, :] = raw[b, at, slot, :]
            return 0

        lax.fori_loop(first, last, turn, 0)

    load = pltpu.make_async_copy(w_hbm, w_ref, w_sem)
    gives = [
        pltpu.make_async_copy(
            out_ref.at[x, pl.ds(t0, tt)], out_hbm.at[x, pl.ds(t0, tt)], out_sem.at[c]
        )
        for c, (x, t0, tt) in enumerate(parts)
    ]

    for c in range(nc):
        for copy in own_blocks(c):
            copy.start()
    for b in seq_order:
        fetches[b].start()
    load.start()
    signalled = greet_start(("tp", "seq"))

    run = dict(
        hello=lambda _: pl.semaphore_wait(pltpu.get_barrier_semaphore(), signalled),
        q=ask_own, ra=relay_a, rb=relay_b, sp=spread, bs=part_send, bj=part_join, be=part_end,
        pr=project, dj=sum_join, de=sum_end, kv=split,
        a0=lambda c: attend(c, 0), a1=lambda c: attend(c, 1),
        a2=lambda c: attend(c, 2), a3=lambda c: attend(c, 3),
    )
    for entry in ORDER:
        name, c = entry.rsplit(".", 1)
        if entry == FIRST_PROJECT:
            load.wait()
        run[name](int(c))

    finish("q", own_p)
    for k in range(1, n_seq):
        finish("sp", xsends[k])
        finish(f"a{k}", osends[k])
        finish(f"a{k}", lsends[k])
        finish("be", gsends[k])
    for name, zs in (("bs", bz), ("pr", dz)):
        for z in zs:
            finish(name, z["pair"])

    @pl.when(outer)
    def _():
        for name, zs in (("bs", bz), ("pr", dz)):
            for z in zs:
                finish(name, z["lift"][1])
                finish(name, z["lift"][2])

    @pl.when(inner)
    def _():
        for name, copies in (("q", own_f), ("ra", via_f), ("ra", via_a), ("rb", via_b)):
            finish(name, copies)
        for name, zs in (("bj", bz), ("dj", dz)):
            for z in zs:
                finish(name, z["cross"][1])
                finish(name, z["cross"][2])

    for c in range(nc):
        gives[c].wait()


def line_call(query, cache, head_of_slot, lengths, out_weight, cuts):
    n_seq, n_tp = lax.axis_size("seq"), lax.axis_size("tp")
    G = HQ // KVH
    B, T, _ = query.shape
    Lb, ns, hd2 = cache.shape[1:]
    hd = hd2 // 2
    hl = KVH // n_tp
    per_tp = B // n_tp
    parts = []
    for x in range(per_tp):
        t0 = 0
        for tt in cuts[x % len(cuts)]:
            parts.append((x, t0, tt))
            t0 += tt
    sizes = [tt for _, _, tt in parts]
    nc = len(parts)
    columns = out_weight.shape[1]
    bf, f32 = jnp.bfloat16, jnp.float32
    dma = pltpu.SemaphoreType.DMA
    v = pltpu.VMEM
    anywhere = pl.BlockSpec(memory_space=pl.ANY)
    smem = pl.BlockSpec(memory_space=pltpu.SMEM)
    return pl.pallas_call(
        functools.partial(line_kernel, (tuple(parts), hl, ns, Lb, hd, G)),
        out_shape=jax.ShapeDtypeStruct((per_tp, T, columns), bf),
        in_specs=[smem, smem, anywhere, anywhere, anywhere],
        out_specs=anywhere,
        scratch_shapes=[
            v(cache.shape, bf),
            v((ns, B, Lb, 2 * hd), bf),
            v(out_weight.shape, bf),
            [v((n_tp, hl, G, tt, hd), bf) for tt in sizes],
            [v((n_seq, ns, G, tt, hd), bf) for tt in sizes],
            [v((n_seq, ns, G, tt, hd), bf) for tt in sizes],
            [v((n_seq, ns, hd, G * tt), bf) for tt in sizes],
            [v((n_seq, ns, hd, G * tt), bf) for tt in sizes],
            [v((n_seq, ns, 1, G * tt), f32) for tt in sizes],
            [v((n_seq, ns, 1, G * tt), f32) for tt in sizes],
            v((Lb, G * max(sizes)), f32),
            [v((3, hl, hd, G * tt), bf) for tt in sizes], [v((3, hl, 1, G * tt), f32) for tt in sizes],
            [v((2, hl, hd, G * tt), bf) for tt in sizes], [v((2, hl, 1, G * tt), f32) for tt in sizes],
            [v((2, hl, hd, G * tt), bf) for tt in sizes], [v((2, hl, 1, G * tt), f32) for tt in sizes],
            [v((n_seq, tt, hl * G * hd), bf) for tt in sizes],
            [v((tt, columns), f32) for tt in sizes],
            [v((3, tt, columns), bf) for tt in sizes],
            [v((2, tt, columns), bf) for tt in sizes],
            [v((2, tt, columns), bf) for tt in sizes],
            dma((B,)), dma(()), dma((nc,)),
            dma((SLOTS, 5)), dma((nc, 3)),
            dma((SLOTS, n_seq - 1)), dma((nc, n_seq - 1)),
            dma((SLOTS, n_seq - 1)), dma((nc, n_seq - 1)),
            dma((SLOTS, n_seq - 1)), dma((nc, n_seq - 1)),
            dma((SLOTS, 5)), dma((nc, 4)), dma((SLOTS, 5)), dma((nc, 4)),
            dma((SLOTS, n_seq - 1)), dma((nc, n_seq - 1)),
            dma((SLOTS, 5)), dma((nc, 4)),
            v((per_tp, T, columns), bf), dma((nc,)),
        ],
        compiler_params=pltpu.CompilerParams(
            collective_id=2, has_side_effects=True, vmem_limit_bytes=60 * 2**20
        ),
    )(head_of_slot, lengths, query, cache, out_weight)


def local(query, cache, head_of_slot, lengths, out_weight):
    G = HQ // KVH
    n_seq, n_tp = lax.axis_size("seq"), lax.axis_size("tp")
    me_s = lax.axis_index("seq")
    slot_of_head = slot_table(head_of_slot)
    B, T, width = query.shape
    Lb, ns, hd2 = cache.shape[1:]
    hd = hd2 // 2
    hl = KVH // n_tp
    per_tp = B // n_tp
    fits = all(sum(cut) == T for cut in CUTS) and len(CUTS) == per_tp
    if n_tp == n_seq == 4 and HQ * hd == n_tp * width and fits:
        return line_call(query, cache, head_of_slot, lengths, out_weight, CUTS)
    nc = math.gcd(CHUNKS, per_tp)
    bq = per_tp // nc
    nsq = n_tp * bq // n_seq
    sub = T // n_seq

    chunked = query.reshape(n_tp, nc, bq, T, width).transpose(1, 0, 2, 3, 4)
    chunked = chunked.reshape(nc, n_seq, nsq, T, width)
    mine = lax.dynamic_index_in_dim(chunked, me_s, 1, False)
    qm = mine.reshape(nc, nsq, T, hl, G, hd).transpose(0, 3, 1, 4, 2, 5)
    kv = cache
    att = gather_attend(
        qm, kv, head_of_slot, lengths, (nc, bq, nsq, hl, ns, per_tp, Lb, hd, G, T)
    )
    att = att.reshape(nc, bq, ns, hd, G, n_seq, sub).transpose(0, 5, 2, 1, 6, 4, 3)
    att = att.reshape(nc, n_seq, ns, bq * sub, G * hd)
    return project(att, out_weight, slot_of_head, (nc, bq, hl, ns, sub, G * hd, T))


def solution(mesh):
    in_specs = (
        P("grp", None, "tp"),
        P("grp", "tp", "seq", None),
        P("grp"),
        P("grp"),
        P("tp", "seq"),
    )
    out_specs = P(("grp", "tp"), None, "seq")
    return jax.shard_map(local, mesh=mesh, in_specs=in_specs, out_specs=out_specs, check_vma=False)
```
